8 devices in a mesh: batch: 1 (over z), pcol: 2 (over y), prow: 4 (over x, core).
Axes of the slice: x: 2, y: 2, z: 1, core: 2. Of those that a mesh axis runs over, the one named last changes fastest.
Arguments:
- a_mat: float32 [24576, 1024], P(('batch', 'prow'), 'pcol')
- diag_shift: float32 [4, 128], P('batch')
Outputs:
- output: float32 [512, 1024], P('batch', 'pcol')
All inputs are finite; a program needn't handle non-finite values.
Results may differ from the reference program's by a relative error of at most 0.001.
Values sent between devices are 32-bit elements.
A program may use at most 1 GiB of HBM per device.

```python
import jax
import jax.numpy as jnp
from jax import lax

ROWS = 24576
COLS = 1024
PCOL = 2
NB = 128
PANELS = 4

COLS_DEV = COLS // PCOL
TOTAL_K = PANELS * NB
PRECISE = lax.Precision.HIGHEST


def stored_to_orig():
    stored = jnp.arange(COLS)
    return ((stored % COLS_DEV) // NB * PCOL + stored // COLS_DEV) * NB + stored % NB


def setup_inputs(seed: int = 0, part: int = 0) -> dict:
    base_key = jax.random.fold_in(jax.random.key(seed), part)
    key_mat, key_sign, key_mag = jax.random.split(base_key, 3)
    gauss_mat = jax.random.normal(key_mat, (ROWS, COLS), jnp.float32)
    col_scale = jnp.where(stored_to_orig() < TOTAL_K, ROWS ** -0.5, 1.0)
    a_mat = gauss_mat * col_scale[None, :]
    shift_sign = jax.random.rademacher(key_sign, (TOTAL_K,), jnp.int32).astype(jnp.float32)
    shift_mag = jax.random.uniform(key_mag, (TOTAL_K,), jnp.float32, 0.4, 0.8)
    diag_shift = (shift_sign * shift_mag).reshape(PANELS, NB)
    return {'a_mat': a_mat, 'diag_shift': diag_shift}


def reference(a_mat, diag_shift):
    orig_cols = stored_to_orig()
    row_ids = jnp.arange(TOTAL_K)
    shift_flat = diag_shift.reshape(TOTAL_K)
    col_shift = jnp.where(orig_cols < TOTAL_K, shift_flat[jnp.minimum(orig_cols, TOTAL_K - 1)], 0.0)
    diag_hit = row_ids[:, None] == orig_cols[None, :]
    shifted = a_mat.at[:TOTAL_K].add(jnp.where(diag_hit, col_shift[None, :], 0.0))
    blocks = row_ids // NB
    first_pos = (blocks % PCOL) * COLS_DEV + (blocks // PCOL) * NB + row_ids % NB
    first_cols = jnp.take(shifted, first_pos, axis=1)
    q_mat, r_mat = jnp.linalg.qr(first_cols)
    row_signs = jnp.where(jnp.diagonal(r_mat) < 0, -1.0, 1.0)
    projected = jnp.einsum('mk,mn->kn', q_mat, shifted, precision=PRECISE)
    projected = jnp.where(orig_cols[None, :] < row_ids[:, None], 0.0, projected)
    return projected * row_signs[:, None]
```

```python
import functools

import jax
import jax.numpy as jnp
from jax import lax
from jax.experimental import pallas as pl
from jax.experimental.pallas import tpu as pltpu
from jax.sharding import PartitionSpec as P

PRECISE = lax.Precision.HIGHEST
F32 = jnp.float32
NB = 128
MESH = pl.DeviceIdType.MESH
TRACE_FACTOR = 2.0


def dot_nn(x, y):
    return lax.dot_general(x, y, (((1,), (0,)), ((), ())), precision=PRECISE, preferred_element_type=F32)


def dot_tn(x, y):
    return lax.dot_general(x, y, (((0,), (0,)), ((), ())), precision=PRECISE, preferred_element_type=F32)


def gather_sum(x, axis):
    return jnp.sum(lax.all_gather(x, axis), axis=0)


def factor_panel(panel, glob_rows, col_base):
    blocksize = panel.shape[1]
    lane_ids = jnp.arange(blocksize)

    def col_step(k, loop_state):
        panel, vectors, tau_vec, sign_vec = loop_state
        glob_col = col_base + k
        active = glob_rows >= glob_col
        is_pivot = glob_rows == glob_col
        column = lax.dynamic_slice_in_dim(panel, k, 1, axis=1)[:, 0]
        reduced = gather_sum(jnp.stack([jnp.sum(jnp.where(active, column, 0.0)[:, None] * panel, axis=0),
                                        jnp.sum(jnp.where(is_pivot[:, None], panel, 0.0), axis=0)]), 'prow')
        col_dots = reduced[0]
        pivot_row = reduced[1]
        pivot_val = lax.dynamic_index_in_dim(pivot_row, k, keepdims=False)
        col_norm = jnp.sqrt(lax.dynamic_index_in_dim(col_dots, k, keepdims=False))
        beta_val = jnp.where(pivot_val >= 0, -col_norm, col_norm)
        tau_val = (beta_val - pivot_val) / beta_val
        inv_scale = 1.0 / (pivot_val - beta_val)
        v_col = jnp.where(is_pivot, 1.0, jnp.where(active, column * inv_scale, 0.0))
        v_dots = inv_scale * (col_dots - pivot_val * pivot_row) + pivot_row
        update = jnp.where(lane_ids > k, tau_val * v_dots, 0.0)
        new_col = jnp.where(active, jnp.where(is_pivot, beta_val, 0.0), column)
        panel = panel - v_col[:, None] * update[None, :]
        panel = lax.dynamic_update_slice_in_dim(panel, new_col[:, None], k, axis=1)
        vectors = lax.dynamic_update_slice_in_dim(vectors, v_col[:, None], k, axis=1)
        tau_vec = jnp.where(lane_ids == k, tau_val, tau_vec)
        sign_vec = jnp.where(lane_ids == k, jnp.where(beta_val < 0, -1.0, 1.0), sign_vec)
        return panel, vectors, tau_vec, sign_vec

    init_state = (panel, jnp.zeros_like(panel), jnp.zeros((blocksize,), F32), jnp.zeros((blocksize,), F32))
    return lax.fori_loop(0, blocksize, col_step, init_state)


def build_tfactor(gram_mat, tau_vec):
    blocksize = tau_vec.shape[0]
    lane_ids = jnp.arange(blocksize)

    def t_step(k, t_factor):
        gram_col = jnp.where(lane_ids < k, lax.dynamic_slice_in_dim(gram_mat, k, 1, axis=1)[:, 0], 0.0)
        tau_k = lax.dynamic_index_in_dim(tau_vec, k, keepdims=False)
        column = -tau_k * jnp.sum(t_factor * gram_col[None, :], axis=1)
        column = jnp.where(lane_ids == k, tau_k, column)
        return jnp.where(lane_ids[None, :] == k, column[:, None], t_factor)

    return lax.fori_loop(0, blocksize, t_step, jnp.zeros((blocksize, blocksize), F32))


def householder_rows(a_loc, diag_shift, n_pcol):
    rows_loc, cols_loc = a_loc.shape
    panels, blocksize = diag_shift.shape
    total_k = panels * blocksize
    row_id = lax.axis_index('prow')
    col_id = lax.axis_index('pcol')
    glob_rows = row_id * rows_loc + jnp.arange(rows_loc)
    local_cols = jnp.arange(cols_loc)
    orig_cols = ((local_cols // blocksize) * n_pcol + col_id) * blocksize + local_cols % blocksize
    shift_flat = diag_shift.reshape(total_k)
    col_shift = jnp.where(orig_cols < total_k, shift_flat[jnp.minimum(orig_cols, total_k - 1)], 0.0)
    a_loc = a_loc + jnp.where(glob_rows[:, None] == orig_cols[None, :], col_shift[None, :], 0.0)
    swap = [(0, 1), (1, 0)]

    def owned(x, is_owner):
        return jnp.where(is_owner, x, lax.ppermute(x, 'pcol', swap))

    def panel_step(panel_idx, state):
        a_loc, signs = state
        owner_col = panel_idx % n_pcol
        start_col = (panel_idx // n_pcol) * blocksize
        is_owner = col_id == owner_col
        panel = lax.dynamic_slice_in_dim(a_loc, start_col, blocksize, axis=1)
        factored, vectors, tau_vec, sign_vec = factor_panel(panel, glob_rows, panel_idx * blocksize)
        gram_mat = gather_sum(jnp.einsum('mi,mj->ij', vectors, vectors, precision=PRECISE, preferred_element_type=F32), 'prow')
        t_factor = build_tfactor(gram_mat, tau_vec)
        vectors, t_factor, sign_vec = owned(vectors, is_owner), owned(t_factor, is_owner), owned(sign_vec, is_owner)
        signs = lax.dynamic_update_slice_in_dim(signs, sign_vec, panel_idx * blocksize, axis=0)
        keep_cols = orig_cols >= (panel_idx + 1) * blocksize
        proj = jnp.einsum('mi,mn->in', vectors, a_loc, precision=PRECISE, preferred_element_type=F32)
        quarter = cols_loc // 4
        proj_sum = jnp.concatenate([gather_sum(proj[:, q * quarter:(q + 1) * quarter], 'prow') for q in range(4)], axis=1)
        w_mat = jnp.where(keep_cols[None, :], jnp.einsum('ij,in->jn', t_factor, proj_sum, precision=PRECISE, preferred_element_type=F32), 0.0)
        a_loc = a_loc - jnp.dot(vectors, w_mat, precision=PRECISE, preferred_element_type=F32)
        kept = lax.dynamic_slice_in_dim(a_loc, start_col, blocksize, axis=1)
        a_loc = lax.dynamic_update_slice_in_dim(a_loc, jnp.where(is_owner, factored, kept), start_col, axis=1)
        return a_loc, signs

    a_loc, signs = lax.fori_loop(0, panels, panel_step, (a_loc, jnp.zeros((total_k,), F32)))
    step = total_k // 8

    def top_step(i, top):
        piece = lax.all_gather(lax.dynamic_slice_in_dim(a_loc, i * step, step, axis=0), 'prow')[0]
        return lax.dynamic_update_slice_in_dim(top, piece, i * step, axis=0)

    top_rows = lax.fori_loop(0, 8, top_step, jnp.zeros((total_k, cols_loc), F32))
    return top_rows * signs[:, None]


def factor_block(block, u_ref, m_ref):
    sub = lax.broadcasted_iota(jnp.int32, (8, NB), 0)
    lane = lax.broadcasted_iota(jnp.int32, (8, NB), 1)
    eye = (lax.broadcasted_iota(jnp.int32, (NB, NB), 0) == lax.broadcasted_iota(jnp.int32, (NB, NB), 1)).astype(F32)

    def group(g, state):
        s_mat, m_mat = state
        for t in range(8):
            row_s = s_mat[t:t + 1, :]
            row_m = m_mat[t:t + 1, :]
            inv_p = 1.0 / s_mat[t:t + 1, t:t + 1]
            row_s = row_s * inv_p
            row_m = row_m * inv_p
            col = s_mat[:, t:t + 1]
            top = jnp.where(sub[:, 0:1] > t, col[:8], 0.0)
            col = jnp.concatenate([top, col[8:]], axis=0)
            s_mat = s_mat - col * row_s
            m_mat = m_mat - col * row_m
        s_top, m_top = s_mat[:8], m_mat[:8]
        diag = jnp.sum(jnp.where(lane == sub, s_top, 0.0), axis=1, keepdims=True)
        scale = 1.0 / jnp.sqrt(diag)
        base = pl.multiple_of(g * 8, 8)
        u_top = pltpu.roll(jnp.where(lane >= sub, s_top * scale, 0.0), base, 1)
        u_ref[pl.ds(base, 8), :] = jnp.where(lane >= sub + base, u_top, 0.0)
        m_ref[pl.ds(base, 8), :] = m_top * scale
        zero = jnp.zeros((8, NB), F32)
        s_mat = pltpu.roll(jnp.concatenate([s_mat[8:], zero], axis=0), NB - 8, 1)
        m_mat = jnp.concatenate([m_mat[8:], zero], axis=0)
        return s_mat, m_mat

    lax.fori_loop(0, NB // 8, group, (block, eye))


def gram_kernel(a_hbm, s_ref, r_hbm, ok_ref, w_buf, y_buf, acc1, acc2, acc1_r, h_buf, cm_buf, cm_recv, cy_recv, cfin,
                xp, xp_r, z_buf, t_buf, rf_buf, k12, r_buf, ymax, u_blk, m_blk,
                load_sem, ya_send, ya_recv, yb_send, yb_recv, ar_send, ar_recv, gy_send, gy_recv, gq_send, gq_recv,
                rs_send, rs_recv, cy_send, cy_rsem, ag_send, ag_recv, out_sem):
    rows, cols = a_hbm.shape
    half_rows = rows // 2
    half = cols // 2
    kk = 2 * half
    c = lax.axis_index('pcol')
    p = lax.axis_index('prow')
    other = 1 - c
    core_peer = p + 1 - 2 * (p % 2)
    x_peer = (p + 2) % 4
    qr = half // 4
    ca = 512
    n_a = half_rows // ca
    cb = 768
    n_b = half_rows // cb
    n_l = rows // ca

    def row0(start, size):
        return pl.ds(pl.multiple_of(start, NB), size)

    def load(j):
        rs = pl.ds(pl.multiple_of(j * ca, ca), ca)
        return (pltpu.make_async_copy(a_hbm.at[rs, pl.ds(0, half)], w_buf.at[c, rs, :], load_sem.at[0, j]),
                pltpu.make_async_copy(a_hbm.at[rs, pl.ds(half, half)], y_buf.at[rs, :], load_sem.at[1, j]))

    for j in range(n_l):
        for cp in load(j):
            cp.start()

    barrier = pltpu.get_barrier_semaphore()
    pl.semaphore_signal(barrier, inc=1, device_id={'pcol': other}, device_id_type=MESH)
    for d in range(1, 4):
        pl.semaphore_signal(barrier, inc=1, device_id={'prow': (p + d) % 4}, device_id_type=MESH)
    pl.semaphore_wait(barrier, 4)

    def send_a(k):
        rs = row0(c * half_rows + k * ca, ca)
        return pltpu.make_async_remote_copy(a_hbm.at[rs, pl.ds(0, half)], w_buf.at[c, rs, :], ya_send.at[k], ya_recv.at[k],
                                            device_id={'pcol': other}, device_id_type=MESH)

    def send_b(l, k):
        rs = row0(other * half_rows + k * cb, cb)
        ls = pl.ds(l * NB, NB)
        return pltpu.make_async_remote_copy(a_hbm.at[rs, ls], w_buf.at[c, rs, ls], yb_send.at[l, k], yb_recv.at[l, k],
                                            device_id={'pcol': other}, device_id_type=MESH)

    for k in range(4):
        send_a(k).start()

    eye = (lax.broadcasted_iota(jnp.int32, (NB, NB), 0) == lax.broadcasted_iota(jnp.int32, (NB, NB), 1)).astype(F32)

    def add_shift(side, l, cond):
        @pl.when(jnp.logical_and(p == 0, cond))
        def _():
            panel = 2 * l + side
            rs = row0(panel * NB, NB)
            w_buf[side, rs, l * NB:(l + 1) * NB] = w_buf[side, rs, l * NB:(l + 1) * NB] + eye * s_ref[pl.ds(panel, 1), :]

    acc1[...] = jnp.zeros_like(acc1)
    acc2[...] = jnp.zeros_like(acc2)
    ymax[...] = jnp.zeros_like(ymax)

    @pl.loop(0, n_l)
    def _(j):
        for cp in load(j):
            cp.wait()
        for l in range(2):
            add_shift(c, l, j == 0)
        rs = pl.ds(pl.multiple_of(j * ca, ca), ca)
        left = w_buf[c, rs, :]
        right = y_buf[rs, :]
        ymax[...] = jnp.maximum(ymax[...], jnp.max(jnp.abs(right).reshape(ca // 8, 8, half), axis=0))
        acc1[...] += dot_tn(left, jnp.concatenate([left, right], axis=1))

    def pair_copy(src, dst, slot, peer):
        return pltpu.make_async_remote_copy(src, dst, ar_send.at[slot], ar_recv.at[slot], device_id={'prow': peer}, device_id_type=MESH)

    g1 = pair_copy(acc1, acc1_r.at[0], 0, core_peer)
    g1.start()
    g1.wait()
    acc1[...] += acc1_r[0]
    g2 = pair_copy(acc1, acc1_r.at[1], 1, x_peer)
    g2.start()
    g2.wait()
    acc1[...] += acc1_r[1]
    h_buf[c] = acc1[:, :half]
    quarter = pl.ds(pl.multiple_of(p * qr, qr), qr)
    gy = pltpu.make_async_remote_copy(h_buf.at[c, quarter, :], h_buf.at[c, quarter, :], gy_send, gy_recv,
                                      device_id={'pcol': other}, device_id_type=MESH)
    gy.start()
    for k in range(4, n_a):
        send_a(k).start()
    send_b(0, 0).start()

    @pl.loop(0, n_a)
    def _(k):
        send_a(k).wait_recv()
        for l in range(2):
            add_shift(other, l, jnp.logical_and(c == 1, k == 0))
        rs = row0(other * half_rows + k * ca, ca)
        right = jnp.concatenate([w_buf[c, rs, :], y_buf[rs, :]], axis=1)
        acc2[...] += dot_tn(w_buf[other, rs, :], right)

        @pl.when(k == n_a - 2)
        def _():
            gy.wait()
            for d in range(1, 4):
                pltpu.make_async_remote_copy(h_buf.at[other, quarter, :], h_buf.at[other, quarter, :], gq_send.at[d], gq_recv.at[d],
                                             device_id={'prow': (p + d) % 4}, device_id_type=MESH).start()

    @pl.when(c == 0)
    def _():
        ct = acc2[:, :half].T
        for q in range(4):
            cm_buf[q, :qr, :] = ct[q * qr:(q + 1) * qr]

    @pl.when(c == 1)
    def _():
        for q in range(4):
            cm_buf[q, :qr, :] = acc2[q * qr:(q + 1) * qr, :half]

    for q in range(4):
        cm_buf[q, qr:, :] = ymax[...]

    def scatter(d):
        q = (p + d) % 4
        return pltpu.make_async_remote_copy(cm_buf.at[q], cm_recv.at[d - 1], rs_send.at[d], rs_recv.at[d],
                                            device_id={'prow': q}, device_id_type=MESH)

    for d in range(1, 4):
        scatter(d).start()
    for l in range(2):
        xp[l] = acc2[l * NB:(l + 1) * NB, half:]
    for d in range(1, 4):
        pltpu.make_async_remote_copy(h_buf.at[other, quarter, :], h_buf.at[other, quarter, :], gq_send.at[d], gq_recv.at[d],
                                     device_id={'prow': (p + d) % 4}, device_id_type=MESH).wait_send()
        src_q = pl.ds(pl.multiple_of(((p + 4 - d) % 4) * qr, qr), qr)
        pltpu.make_async_remote_copy(h_buf.at[other, src_q, :], h_buf.at[other, src_q, :], gq_send.at[d], gq_recv.at[d],
                                     device_id={'prow': (p + d) % 4}, device_id_type=MESH).wait_recv()
    for d in range(1, 4):
        scatter(d).wait()
    cm_buf[p] = ((cm_buf[p] + cm_recv[0]) + cm_recv[1]) + cm_recv[2]
    cy = pltpu.make_async_remote_copy(cm_buf.at[p], cy_recv, cy_send, cy_rsem, device_id={'pcol': other}, device_id_type=MESH)
    cy.start()
    for k in range(1, n_b):
        send_b(0, k).start()
    for k in range(n_b):
        send_b(1, k).start()
    cy.wait()
    cfin[p] = cm_buf[p] + cy_recv[...]

    def spread(d, src):
        return pltpu.make_async_remote_copy(cfin.at[src], cfin.at[src], ag_send.at[d], ag_recv.at[d],
                                            device_id={'prow': (p + d) % 4}, device_id_type=MESH)

    for d in range(1, 4):
        spread(d, p).start()

    factor_block(h_buf[0, :NB, :NB], u_blk, m_blk)

    for d in range(1, 4):
        spread(d, p).wait_send()
        spread(d, (p + 4 - d) % 4).wait_recv()

    cross = jnp.concatenate([cfin[q, :qr, :] for q in range(4)], axis=0)
    z_buf[...] = jnp.zeros_like(z_buf)
    diag_max = jnp.zeros((1, NB), F32)
    diag_min = jnp.full((1, NB), jnp.inf, F32)
    diags = []
    for i in range(4):
        ci, li = i % 2, i // 2
        for j in range(i, 4):
            cj, lj = j % 2, j // 2
            if ci == cj:
                block = h_buf[ci, li * NB:(li + 1) * NB, lj * NB:(lj + 1) * NB]
            elif ci == 0:
                block = cross[li * NB:(li + 1) * NB, lj * NB:(lj + 1) * NB]
            else:
                block = cross[lj * NB:(lj + 1) * NB, li * NB:(li + 1) * NB].T
            z_buf[i * NB:(i + 1) * NB, j * NB:(j + 1) * NB] = block
            if i == j:
                d_row = jnp.sum(block * eye, axis=0, keepdims=True)
                diags.append(d_row)
                diag_max = jnp.maximum(diag_max, d_row)
                diag_min = jnp.minimum(diag_min, d_row)

    t_buf[...] = jnp.zeros_like(t_buf)
    rf_buf[...] = jnp.zeros_like(rf_buf)
    for j in range(4):
        lo, hi = j * NB, (j + 1) * NB
        if j > 0:
            factor_block(z_buf[lo:hi, lo:hi], u_blk, m_blk)
        inv_t = m_blk[...]
        rf_buf[lo:hi, lo:hi] = u_blk[...]
        t_buf[lo:hi, lo:hi] = inv_t
        new_row = dot_nn(inv_t, z_buf[lo:hi, :])
        if j > 0:
            t_buf[lo:hi, :lo] = new_row[:, :lo]
        if j < 3:
            rf_buf[lo:hi, hi:] = new_row[:, hi:]
            parts = ([new_row[:, :lo]] if j > 0 else []) + [inv_t, new_row[:, hi:]]
            mult = jnp.concatenate(parts, axis=1)
            z_buf[hi:, lo:hi] = jnp.zeros((kk - hi, NB), F32)
            z_buf[hi:, :] = z_buf[hi:, :] - dot_tn(new_row[:, hi:], mult)

    trace = jnp.zeros((1, NB), F32)
    for i in range(4):
        tc = t_buf[i * NB:, i * NB:(i + 1) * NB]
        trace = trace + jnp.sum(tc * tc, axis=0, keepdims=True) * diags[i]
    total = jnp.sum(trace, axis=1, keepdims=True)
    d_max = jnp.max(diag_max, axis=1, keepdims=True)
    d_min = jnp.min(diag_min, axis=1, keepdims=True)
    y_max = jnp.max(jnp.max(cfin[0, qr:, :], axis=0, keepdims=True), axis=1, keepdims=True)
    good = (total < TRACE_FACTOR * kk) & (d_min > 1e-26) & (d_max < 1e36) & (y_max * jnp.sqrt(d_max) < 1e33)
    ok_ref[...] = jnp.broadcast_to(jnp.where(good, 1.0, 0.0), ok_ref.shape)

    for l in range(2):
        ls = pl.ds(pl.multiple_of((2 * l + c) * NB, NB), NB)
        r_buf[:, l * NB:(l + 1) * NB] = rf_buf[:, ls]

    k12[row0(c * NB, NB), :] = acc1[:NB, half:]
    k12[row0((c + 2) * NB, NB), :] = acc1[NB:, half:]
    k12[row0((3 - c) * NB, NB), :] = jnp.zeros((NB, half), F32)

    def take_b(l, k):
        send_b(l, k).wait_recv()
        if k == 0:
            add_shift(other, l, c == 0)
        rs = row0(c * half_rows + k * cb, cb)
        xp[l] += dot_tn(w_buf[other, rs, l * NB:(l + 1) * NB], y_buf[rs, :])

    for k in range(n_b):
        take_b(0, k)
    x1 = pair_copy(xp.at[0], xp_r.at[0], 2, core_peer)
    x1.start()
    x1.wait()
    xp[0] = xp[0] + xp_r[0]
    x2 = pair_copy(xp.at[0], xp_r.at[1], 3, x_peer)
    x2.start()
    take_b(1, 0)
    x2.wait()
    k12[row0((1 - c) * NB, NB), :] = xp[0] + xp_r[1]
    r_buf[:, half:] = dot_nn(t_buf[...], k12[...])
    for k in range(1, n_b):
        take_b(1, k)
    x3 = pair_copy(xp.at[1], xp_r.at[2], 4, core_peer)
    x3.start()
    x3.wait()
    xp[1] = xp[1] + xp_r[2]
    x4 = pair_copy(xp.at[1], xp_r.at[3], 5, x_peer)
    x4.start()
    x4.wait()
    last = xp[1] + xp_r[3]
    r_buf[half:, half:] += dot_nn(t_buf[half:, pl.ds(pl.multiple_of((3 - c) * NB, NB), NB)], last)
    out = pltpu.make_async_copy(r_buf, r_hbm, out_sem)
    out.start()

    for k in range(n_a):
        send_a(k).wait_send()
    for l in range(2):
        for k in range(n_b):
            send_b(l, k).wait_send()
    out.wait()


def gram_rows(a_loc, diag_shift):
    rows, cols = a_loc.shape
    half = cols // 2
    kk = cols
    qr = half // 4
    dma = pltpu.SemaphoreType.DMA
    vm = lambda *shape: pltpu.VMEM(shape, F32)
    return pl.pallas_call(
        gram_kernel,
        out_shape=(jax.ShapeDtypeStruct((kk, cols), F32), jax.ShapeDtypeStruct((8, NB), F32)),
        in_specs=[pl.BlockSpec(memory_space=pl.ANY), pl.BlockSpec(memory_space=pltpu.VMEM)],
        out_specs=(pl.BlockSpec(memory_space=pl.ANY), pl.BlockSpec(memory_space=pltpu.VMEM)),
        scratch_shapes=[
            vm(2, rows, half), vm(rows, half), vm(half, cols), vm(half, cols), vm(2, half, cols), vm(2, half, half),
            vm(4, qr + 8, half), vm(3, qr + 8, half), vm(qr + 8, half), vm(4, qr + 8, half),
            vm(2, NB, half), vm(4, NB, half), vm(kk, kk), vm(kk, kk), vm(kk, kk), vm(kk, half), vm(kk, cols), vm(8, half),
            vm(NB, NB), vm(NB, NB),
            dma((2, rows // 512)), dma((rows // 1024,)), dma((rows // 1024,)), dma((2, rows // 1536)), dma((2, rows // 1536)),
            dma((6,)), dma((6,)), dma, dma, dma((4,)), dma((4,)),
            dma((4,)), dma((4,)), dma, dma, dma((4,)), dma((4,)), dma,
        ],
        compiler_params=pltpu.CompilerParams(collective_id=0, has_side_effects=True, vmem_limit_bytes=56 * 1024 * 1024),
        name='gram_rows',
    )(a_loc, diag_shift)


def solution(mesh):
    n_pcol = mesh.shape['pcol']

    def local_qr(a_loc, diag_shift):
        rows, ok = gram_rows(a_loc, diag_shift)
        return lax.cond(ok[0, 0] > 0.5, lambda a, s, r: r, lambda a, s, r: householder_rows(a, s, n_pcol), a_loc, diag_shift, rows)

    return jax.shard_map(local_qr, mesh=mesh, in_specs=(P(('batch', 'prow'), 'pcol'), P('batch', None)), out_specs=P('batch', 'pcol'), check_vma=False)
```

```python
import functools

import jax
import jax.numpy as jnp
from jax import lax
from jax.experimental import pallas as pl
from jax.experimental.pallas import tpu as pltpu
from jax.sharding import PartitionSpec as P

PRECISE = lax.Precision.HIGHEST
F32 = jnp.float32
NB = 128
MESH = pl.DeviceIdType.MESH
TRACE_FACTOR = 2.0


def dot_nn(x, y):
    return lax.dot_general(x, y, (((1,), (0,)), ((), ())), precision=PRECISE, preferred_element_type=F32)


def dot_tn(x, y):
    return lax.dot_general(x, y, (((0,), (0,)), ((), ())), precision=PRECISE, preferred_element_type=F32)


def gather_sum(x, axis):
    return jnp.sum(lax.all_gather(x, axis), axis=0)


def factor_panel(panel, glob_rows, col_base):
    blocksize = panel.shape[1]
    lane_ids = jnp.arange(blocksize)

    def col_step(k, loop_state):
        panel, vectors, tau_vec, sign_vec = loop_state
        glob_col = col_base + k
        active = glob_rows >= glob_col
        is_pivot = glob_rows == glob_col
        column = lax.dynamic_slice_in_dim(panel, k, 1, axis=1)[:, 0]
        reduced = gather_sum(jnp.stack([jnp.sum(jnp.where(active, column, 0.0)[:, None] * panel, axis=0),
                                        jnp.sum(jnp.where(is_pivot[:, None], panel, 0.0), axis=0)]), 'prow')
        col_dots = reduced[0]
        pivot_row = reduced[1]
        pivot_val = lax.dynamic_index_in_dim(pivot_row, k, keepdims=False)
        col_norm = jnp.sqrt(lax.dynamic_index_in_dim(col_dots, k, keepdims=False))
        beta_val = jnp.where(pivot_val >= 0, -col_norm, col_norm)
        tau_val = (beta_val - pivot_val) / beta_val
        inv_scale = 1.0 / (pivot_val - beta_val)
        v_col = jnp.where(is_pivot, 1.0, jnp.where(active, column * inv_scale, 0.0))
        v_dots = inv_scale * (col_dots - pivot_val * pivot_row) + pivot_row
        update = jnp.where(lane_ids > k, tau_val * v_dots, 0.0)
        new_col = jnp.where(active, jnp.where(is_pivot, beta_val, 0.0), column)
        panel = panel - v_col[:, None] * update[None, :]
        panel = lax.dynamic_update_slice_in_dim(panel, new_col[:, None], k, axis=1)
        vectors = lax.dynamic_update_slice_in_dim(vectors, v_col[:, None], k, axis=1)
        tau_vec = jnp.where(lane_ids == k, tau_val, tau_vec)
        sign_vec = jnp.where(lane_ids == k, jnp.where(beta_val < 0, -1.0, 1.0), sign_vec)
        return panel, vectors, tau_vec, sign_vec

    init_state = (panel, jnp.zeros_like(panel), jnp.zeros((blocksize,), F32), jnp.zeros((blocksize,), F32))
    return lax.fori_loop(0, blocksize, col_step, init_state)


def build_tfactor(gram_mat, tau_vec):
    blocksize = tau_vec.shape[0]
    lane_ids = jnp.arange(blocksize)

    def t_step(k, t_factor):
        gram_col = jnp.where(lane_ids < k, lax.dynamic_slice_in_dim(gram_mat, k, 1, axis=1)[:, 0], 0.0)
        tau_k = lax.dynamic_index_in_dim(tau_vec, k, keepdims=False)
        column = -tau_k * jnp.sum(t_factor * gram_col[None, :], axis=1)
        column = jnp.where(lane_ids == k, tau_k, column)
        return jnp.where(lane_ids[None, :] == k, column[:, None], t_factor)

    return lax.fori_loop(0, blocksize, t_step, jnp.zeros((blocksize, blocksize), F32))


def householder_rows(a_loc, diag_shift, n_pcol):
    rows_loc, cols_loc = a_loc.shape
    panels, blocksize = diag_shift.shape
    total_k = panels * blocksize
    row_id = lax.axis_index('prow')
    col_id = lax.axis_index('pcol')
    glob_rows = row_id * rows_loc + jnp.arange(rows_loc)
    local_cols = jnp.arange(cols_loc)
    orig_cols = ((local_cols // blocksize) * n_pcol + col_id) * blocksize + local_cols % blocksize
    shift_flat = diag_shift.reshape(total_k)
    col_shift = jnp.where(orig_cols < total_k, shift_flat[jnp.minimum(orig_cols, total_k - 1)], 0.0)
    a_loc = a_loc + jnp.where(glob_rows[:, None] == orig_cols[None, :], col_shift[None, :], 0.0)
    swap = [(0, 1), (1, 0)]

    def owned(x, is_owner):
        return jnp.where(is_owner, x, lax.ppermute(x, 'pcol', swap))

    def panel_step(panel_idx, state):
        a_loc, signs = state
        owner_col = panel_idx % n_pcol
        start_col = (panel_idx // n_pcol) * blocksize
        is_owner = col_id == owner_col
        panel = lax.dynamic_slice_in_dim(a_loc, start_col, blocksize, axis=1)
        factored, vectors, tau_vec, sign_vec = factor_panel(panel, glob_rows, panel_idx * blocksize)
        gram_mat = gather_sum(jnp.einsum('mi,mj->ij', vectors, vectors, precision=PRECISE, preferred_element_type=F32), 'prow')
        t_factor = build_tfactor(gram_mat, tau_vec)
        vectors, t_factor, sign_vec = owned(vectors, is_owner), owned(t_factor, is_owner), owned(sign_vec, is_owner)
        signs = lax.dynamic_update_slice_in_dim(signs, sign_vec, panel_idx * blocksize, axis=0)
        keep_cols = orig_cols >= (panel_idx + 1) * blocksize
        proj = jnp.einsum('mi,mn->in', vectors, a_loc, precision=PRECISE, preferred_element_type=F32)
        quarter = cols_loc // 4
        proj_sum = jnp.concatenate([gather_sum(proj[:, q * quarter:(q + 1) * quarter], 'prow') for q in range(4)], axis=1)
        w_mat = jnp.where(keep_cols[None, :], jnp.einsum('ij,in->jn', t_factor, proj_sum, precision=PRECISE, preferred_element_type=F32), 0.0)
        a_loc = a_loc - jnp.dot(vectors, w_mat, precision=PRECISE, preferred_element_type=F32)
        kept = lax.dynamic_slice_in_dim(a_loc, start_col, blocksize, axis=1)
        a_loc = lax.dynamic_update_slice_in_dim(a_loc, jnp.where(is_owner, factored, kept), start_col, axis=1)
        return a_loc, signs

    a_loc, signs = lax.fori_loop(0, panels, panel_step, (a_loc, jnp.zeros((total_k,), F32)))
    step = total_k // 8

    def top_step(i, top):
        piece = lax.all_gather(lax.dynamic_slice_in_dim(a_loc, i * step, step, axis=0), 'prow')[0]
        return lax.dynamic_update_slice_in_dim(top, piece, i * step, axis=0)

    top_rows = lax.fori_loop(0, 8, top_step, jnp.zeros((total_k, cols_loc), F32))
    return top_rows * signs[:, None]


def factor_block(block, u_ref, m_ref):
    sub = lax.broadcasted_iota(jnp.int32, (8, NB), 0)
    lane = lax.broadcasted_iota(jnp.int32, (8, NB), 1)
    eye = (lax.broadcasted_iota(jnp.int32, (NB, NB), 0) == lax.broadcasted_iota(jnp.int32, (NB, NB), 1)).astype(F32)
    wide = lambda row: jnp.broadcast_to(row, (8, NB))

    def group(tiles, g, state):
        s_tiles, m_tiles = state[:tiles], state[tiles:]
        base = pl.multiple_of(g * 8, 8)
        spread = lambda tile, t: jnp.take_along_axis(tile, jnp.full((8, NB), base + t, jnp.int32), axis=1)
        s_top, m_top = s_tiles[0], m_tiles[0]
        cols = [spread(s_top, t) for t in range(8)]
        dinv = jnp.zeros((8, NB), F32)
        for s in range(8):
            inv_p = 1.0 / wide(cols[s][s:s + 1])
            dinv = jnp.where(sub == s, inv_p, dinv)
            mult = jnp.where(sub > s, cols[s] * inv_p, 0.0)
            for t in range(s + 1, 8):
                cols[t] = cols[t] - mult * wide(cols[t][s:s + 1])
            s_top = s_top - mult * wide(s_top[s:s + 1])
            m_top = m_top - mult * wide(m_top[s:s + 1])
        scale = jnp.sqrt(dinv)
        u_ref[pl.ds(base, 8), :] = jnp.where(lane >= sub + base, s_top * scale, 0.0)
        m_ref[pl.ds(base, 8), :] = m_top * scale
        s_sol, m_sol = s_top * dinv, m_top * dinv
        for s in range(7, 0, -1):
            mult = jnp.where(sub < s, cols[s] * dinv, 0.0)
            s_sol = s_sol - mult * wide(s_sol[s:s + 1])
            m_sol = m_sol - mult * wide(m_sol[s:s + 1])
        s_rows = [wide(s_sol[t:t + 1]) for t in range(8)]
        m_rows = [wide(m_sol[t:t + 1]) for t in range(8)]
        s_new, m_new = [], []
        for v in range(1, tiles):
            s_acc, m_acc = s_tiles[v], m_tiles[v]
            for t in range(8):
                col = spread(s_tiles[v], t)
                s_acc = s_acc - col * s_rows[t]
                m_acc = m_acc - col * m_rows[t]
            s_new.append(s_acc)
            m_new.append(m_acc)
        zero = jnp.zeros((8, NB), F32)
        return tuple(s_new + [zero] + m_new + [zero])

    def tiles_of(x):
        return [x[8 * v:8 * v + 8] for v in range(x.shape[0] // 8)]

    n = NB // 8
    state = tuple(tiles_of(block) + tiles_of(eye))
    done = 0
    for tiles, steps in ((n, n // 2), (n // 2, n // 2)):
        state = lax.fori_loop(done, done + steps, functools.partial(group, tiles), state)
        done += steps
        half = len(state) // 2
        state = state[:n - done] + state[half:half + n - done]


def gram_kernel(a_hbm, s_hbm, r_hbm, ok_hbm, s_ref, ok_ref, w_buf, y_buf, acc1, acc2, acc1_r, h_buf, cm_buf, cm_recv, cy_recv, cfin,
                xp, xp_r, tail_r, tail_s, last_buf, z_buf, t_buf, rf_buf, k12, r_buf, ymax, u_blk, m_blk,
                load_sem, ya_send, ya_recv, yb_send, yb_recv, ar_send, ar_recv, gy_send, gy_recv, gq_send, gq_recv,
                rs_send, rs_recv, cy_send, cy_rsem, ag_send, ag_recv, s_sem, out_sem):
    rows, cols = a_hbm.shape
    half_rows = rows // 2
    half = cols // 2
    kk = 2 * half
    c = lax.axis_index('pcol')
    p = lax.axis_index('prow')
    other = 1 - c
    core_peer = p + 1 - 2 * (p % 2)
    x_peer = (p + 2) % 4
    qr = half // 4
    ca = 512
    n_a = half_rows // ca
    b_cuts = ((0, 768, 1920, 3072), (0, 1024, 2048, 2816, 3072))
    n_b = [len(cuts) - 1 for cuts in b_cuts]
    n_l = rows // ca

    def row0(start, size):
        return pl.ds(pl.multiple_of(start, NB), size)

    def load(j):
        rs = pl.ds(pl.multiple_of(j * ca, ca), ca)
        return (pltpu.make_async_copy(a_hbm.at[rs, pl.ds(0, half)], w_buf.at[c, rs, :], load_sem.at[0, j]),
                pltpu.make_async_copy(a_hbm.at[rs, pl.ds(half, half)], y_buf.at[rs, :], load_sem.at[1, j]))

    barrier = pltpu.get_barrier_semaphore()
    pl.semaphore_signal(barrier, inc=1, device_id={'pcol': other}, device_id_type=MESH)
    for d in range(1, 4):
        pl.semaphore_signal(barrier, inc=1, device_id={'prow': (p + d) % 4}, device_id_type=MESH)
    s_load = pltpu.make_async_copy(s_hbm, s_ref, s_sem)
    s_load.start()
    for j in range(n_l):
        for cp in load(j):
            cp.start()
    pl.semaphore_wait(barrier, 4)

    def send_a(k):
        rs = row0(c * half_rows + k * ca, ca)
        return pltpu.make_async_remote_copy(a_hbm.at[rs, pl.ds(0, half)], w_buf.at[c, rs, :], ya_send.at[k], ya_recv.at[k],
                                            device_id={'pcol': other}, device_id_type=MESH)

    def send_b(l, k):
        rs = row0(other * half_rows + b_cuts[l][k], b_cuts[l][k + 1] - b_cuts[l][k])
        ls = pl.ds(l * NB, NB)
        return pltpu.make_async_remote_copy(a_hbm.at[rs, ls], w_buf.at[c, rs, ls], yb_send.at[l, k], yb_recv.at[l, k],
                                            device_id={'pcol': other}, device_id_type=MESH)

    for k in range(4):
        send_a(k).start()

    eye = (lax.broadcasted_iota(jnp.int32, (NB, NB), 0) == lax.broadcasted_iota(jnp.int32, (NB, NB), 1)).astype(F32)

    def add_shift(side, l, cond):
        @pl.when(jnp.logical_and(p == 0, cond))
        def _():
            panel = 2 * l + side
            rs = row0(panel * NB, NB)
            w_buf[side, rs, l * NB:(l + 1) * NB] = w_buf[side, rs, l * NB:(l + 1) * NB] + eye * s_ref[pl.ds(panel, 1), :]

    acc1[...] = jnp.zeros_like(acc1)
    acc2[...] = jnp.zeros_like(acc2)
    ymax[...] = jnp.zeros_like(ymax)
    s_load.wait()

    @pl.loop(0, n_l)
    def _(j):
        for cp in load(j):
            cp.wait()
        for l in range(2):
            add_shift(c, l, j == 0)
        rs = pl.ds(pl.multiple_of(j * ca, ca), ca)
        left = w_buf[c, rs, :]
        right = y_buf[rs, :]
        ymax[...] = jnp.maximum(ymax[...], jnp.max(jnp.abs(right).reshape(ca // 8, 8, half), axis=0))
        acc1[...] += dot_tn(left, jnp.concatenate([left, right], axis=1))

    def pair_copy(src, dst, slot, peer):
        return pltpu.make_async_remote_copy(src, dst, ar_send.at[slot], ar_recv.at[slot], device_id={'prow': peer}, device_id_type=MESH)

    g1 = pair_copy(acc1, acc1_r.at[0], 0, core_peer)
    g1.start()
    g1.wait()
    acc1[...] += acc1_r[0]
    g2 = pair_copy(acc1, acc1_r.at[1], 1, x_peer)
    g2.start()
    g2.wait()
    acc1[...] += acc1_r[1]
    h_buf[c] = acc1[:, :half]
    quarter = pl.ds(pl.multiple_of(p * qr, qr), qr)
    gy = pltpu.make_async_remote_copy(h_buf.at[c, quarter, :], h_buf.at[c, quarter, :], gy_send, gy_recv,
                                      device_id={'pcol': other}, device_id_type=MESH)
    gy.start()
    for k in range(4, n_a):
        send_a(k).start()
    send_b(0, 0).start()

    def take_a(k):
        send_a(k).wait_recv()
        for l in range(2):
            add_shift(other, l, jnp.logical_and(c == 1, k == 0))
        rs = row0(other * half_rows + k * ca, ca)
        right = jnp.concatenate([w_buf[c, rs, :], y_buf[rs, :]], axis=1)
        acc2[...] += dot_tn(w_buf[other, rs, :], right)

    def spread_gram(d, src):
        rs = pl.ds(pl.multiple_of(src * qr, qr), qr)
        return pltpu.make_async_remote_copy(h_buf.at[other, rs, :], h_buf.at[other, rs, :], gq_send.at[d], gq_recv.at[d],
                                            device_id={'prow': (p + d) % 4}, device_id_type=MESH)

    @pl.loop(0, n_a)
    def _(k):
        take_a(k)

        @pl.when(k == n_a - 3)
        def _():
            gy.wait()
            for d in range(1, 4):
                spread_gram(d, p).start()

        @pl.when(k == n_a - 2)
        def _():
            for d in range(1, 4):
                spread_gram(d, p).wait_send()
                spread_gram(d, (p + 4 - d) % 4).wait_recv()
            factor_block(h_buf[0, :NB, :NB], u_blk, m_blk)

    @pl.when(c == 0)
    def _():
        ct = acc2[:, :half].T
        for q in range(4):
            cm_buf[q, :qr, :] = ct[q * qr:(q + 1) * qr]

    @pl.when(c == 1)
    def _():
        for q in range(4):
            cm_buf[q, :qr, :] = acc2[q * qr:(q + 1) * qr, :half]

    for q in range(4):
        cm_buf[q, qr:, :] = ymax[...]

    def scatter(d):
        q = (p + d) % 4
        return pltpu.make_async_remote_copy(cm_buf.at[q], cm_recv.at[d - 1], rs_send.at[d], rs_recv.at[d],
                                            device_id={'prow': q}, device_id_type=MESH)

    for d in range(1, 4):
        scatter(d).start()
    for l in range(2):
        xp[l] = acc2[l * NB:(l + 1) * NB, half:]
    for d in range(1, 4):
        scatter(d).wait()
    cm_buf[p] = ((cm_buf[p] + cm_recv[0]) + cm_recv[1]) + cm_recv[2]
    cy = pltpu.make_async_remote_copy(cm_buf.at[p], cy_recv, cy_send, cy_rsem, device_id={'pcol': other}, device_id_type=MESH)
    cy.start()
    for k in range(1, n_b[0]):
        send_b(0, k).start()
    for k in range(n_b[1]):
        send_b(1, k).start()
    cy.wait()
    cfin[p] = cm_buf[p] + cy_recv[...]

    def spread(d, src):
        return pltpu.make_async_remote_copy(cfin.at[src], cfin.at[src], ag_send.at[d], ag_recv.at[d],
                                            device_id={'prow': (p + d) % 4}, device_id_type=MESH)

    for d in range(1, 4):
        spread(d, p).start()

    for d in range(1, 4):
        spread(d, p).wait_send()
        spread(d, (p + 4 - d) % 4).wait_recv()

    cross = jnp.concatenate([cfin[q, :qr, :] for q in range(4)], axis=0)
    z_buf[...] = jnp.zeros_like(z_buf)
    diag_max = jnp.zeros((1, NB), F32)
    diag_min = jnp.full((1, NB), jnp.inf, F32)
    diags = []
    for i in range(4):
        ci, li = i % 2, i // 2
        for j in range(i, 4):
            cj, lj = j % 2, j // 2
            if ci == cj:
                block = h_buf[ci, li * NB:(li + 1) * NB, lj * NB:(lj + 1) * NB]
            elif ci == 0:
                block = cross[li * NB:(li + 1) * NB, lj * NB:(lj + 1) * NB]
            else:
                block = cross[lj * NB:(lj + 1) * NB, li * NB:(li + 1) * NB].T
            z_buf[i * NB:(i + 1) * NB, j * NB:(j + 1) * NB] = block
            if i == j:
                d_row = jnp.sum(block * eye, axis=0, keepdims=True)
                diags.append(d_row)
                diag_max = jnp.maximum(diag_max, d_row)
                diag_min = jnp.minimum(diag_min, d_row)

    t_buf[...] = jnp.zeros_like(t_buf)
    rf_buf[...] = jnp.zeros_like(rf_buf)
    for j in range(4):
        lo, hi = j * NB, (j + 1) * NB
        if j > 0:
            factor_block(z_buf[lo:hi, lo:hi], u_blk, m_blk)
        inv_t = m_blk[...]
        rf_buf[lo:hi, lo:hi] = u_blk[...]
        t_buf[lo:hi, lo:hi] = inv_t
        new_row = dot_nn(inv_t, z_buf[lo:hi, :])
        if j > 0:
            t_buf[lo:hi, :lo] = new_row[:, :lo]
        if j < 3:
            rf_buf[lo:hi, hi:] = new_row[:, hi:]
            parts = ([new_row[:, :lo]] if j > 0 else []) + [inv_t, new_row[:, hi:]]
            mult = jnp.concatenate(parts, axis=1)
            z_buf[hi:, lo:hi] = jnp.zeros((kk - hi, NB), F32)
            z_buf[hi:, :] = z_buf[hi:, :] - dot_tn(new_row[:, hi:], mult)

    trace = jnp.zeros((1, NB), F32)
    for i in range(4):
        tc = t_buf[i * NB:, i * NB:(i + 1) * NB]
        trace = trace + jnp.sum(tc * tc, axis=0, keepdims=True) * diags[i]
    total = jnp.sum(trace, axis=1, keepdims=True)
    d_max = jnp.max(diag_max, axis=1, keepdims=True)
    d_min = jnp.min(diag_min, axis=1, keepdims=True)
    y_max = jnp.max(jnp.max(cfin[0, qr:, :], axis=0, keepdims=True), axis=1, keepdims=True)
    good = (total < TRACE_FACTOR * kk) & (d_min > 1e-26) & (d_max < 1e36) & (y_max * jnp.sqrt(d_max) < 1e33)
    ok_ref[...] = jnp.broadcast_to(jnp.where(good, 1.0, 0.0), ok_ref.shape)
    ok_out = pltpu.make_async_copy(ok_ref, ok_hbm, out_sem.at[0])
    ok_out.start()

    for l in range(2):
        ls = pl.ds(pl.multiple_of((2 * l + c) * NB, NB), NB)
        r_buf[:, l * NB:(l + 1) * NB] = rf_buf[:, ls]

    def out_copy(i, rows_i, cols_i):
        return pltpu.make_async_copy(r_buf.at[rows_i, cols_i], r_hbm.at[rows_i, cols_i], out_sem.at[i])

    outs = [out_copy(1, pl.ds(0, kk), pl.ds(0, half)), out_copy(2, pl.ds(0, half), pl.ds(half, half)),
            out_copy(3, pl.ds(half, half), pl.ds(half, half))]
    outs[0].start()

    k12[row0(c * NB, NB), :] = acc1[:NB, half:]
    k12[row0((c + 2) * NB, NB), :] = acc1[NB:, half:]
    k12[row0((3 - c) * NB, NB), :] = jnp.zeros((NB, half), F32)

    def take_b(l, k):
        send_b(l, k).wait_recv()
        if k == 0:
            add_shift(other, l, c == 0)
        rs = row0(c * half_rows + b_cuts[l][k], b_cuts[l][k + 1] - b_cuts[l][k])
        xp[l] += dot_tn(w_buf[other, rs, l * NB:(l + 1) * NB], y_buf[rs, :])

    for k in range(n_b[0]):
        take_b(0, k)
    x1 = pair_copy(xp.at[0], xp_r.at[0], 2, core_peer)
    x1.start()
    x1.wait()
    xp[0] = xp[0] + xp_r[0]
    x2 = pair_copy(xp.at[0], xp_r.at[1], 3, x_peer)
    x2.start()
    x2.wait()
    k12[row0((1 - c) * NB, NB), :] = xp[0] + xp_r[1]
    r_buf[:, half:] = dot_nn(t_buf[...], k12[...])
    outs[1].start()
    for k in range(n_b[1]):
        take_b(1, k)
    mine = pl.ds(pl.multiple_of((p % 2) * (NB // 2), NB // 2), NB // 2)
    theirs = pl.ds(pl.multiple_of((1 - p % 2) * (NB // 2), NB // 2), NB // 2)
    x3 = pair_copy(xp.at[1, theirs, :], tail_r.at[0], 4, core_peer)
    x3.start()
    x3.wait()
    tail_s[...] = xp[1, mine, :] + tail_r[0]
    x4 = pair_copy(tail_s, tail_r.at[1], 5, x_peer)
    x4.start()
    x4.wait()
    last_buf[mine, :] = tail_s[...] + tail_r[1]
    x5 = pair_copy(last_buf.at[mine, :], last_buf.at[mine, :], 6, core_peer)
    x5.start()
    x5.wait()
    r_buf[half:, half:] += dot_nn(t_buf[half:, pl.ds(pl.multiple_of((3 - c) * NB, NB), NB)], last_buf[...])
    outs[2].start()

    for k in range(n_a):
        send_a(k).wait_send()
    for l in range(2):
        for k in range(n_b[l]):
            send_b(l, k).wait_send()
    ok_out.wait()
    for out in outs:
        out.wait()


def gram_rows(a_loc, diag_shift):
    rows, cols = a_loc.shape
    half = cols // 2
    kk = cols
    qr = half // 4
    dma = pltpu.SemaphoreType.DMA
    vm = lambda *shape: pltpu.VMEM(shape, F32)
    return pl.pallas_call(
        gram_kernel,
        out_shape=(jax.ShapeDtypeStruct((kk, cols), F32), jax.ShapeDtypeStruct((8, NB), F32)),
        in_specs=[pl.BlockSpec(memory_space=pl.ANY), pl.BlockSpec(memory_space=pl.ANY)],
        out_specs=(pl.BlockSpec(memory_space=pl.ANY), pl.BlockSpec(memory_space=pl.ANY)),
        scratch_shapes=[
            vm(*diag_shift.shape), vm(8, NB),
            vm(2, rows, half), vm(rows, half), vm(half, cols), vm(half, cols), vm(2, half, cols), vm(2, half, half),
            vm(4, qr + 8, half), vm(3, qr + 8, half), vm(qr + 8, half), vm(4, qr + 8, half),
            vm(2, NB, half), vm(2, NB, half), vm(2, NB // 2, half), vm(NB // 2, half), vm(NB, half), vm(kk, kk), vm(kk, kk), vm(kk, kk), vm(kk, half), vm(kk, cols), vm(8, half),
            vm(NB, NB), vm(NB, NB),
            dma((2, rows // 512)), dma((rows // 1024,)), dma((rows // 1024,)), dma((2, 4)), dma((2, 4)),
            dma((7,)), dma((7,)), dma, dma, dma((4,)), dma((4,)),
            dma((4,)), dma((4,)), dma, dma, dma((4,)), dma((4,)), dma, dma((4,)),
        ],
        compiler_params=pltpu.CompilerParams(collective_id=0, has_side_effects=True, vmem_limit_bytes=56 * 1024 * 1024),
        name='gram_rows',
    )(a_loc, diag_shift)


def solution(mesh):
    n_pcol = mesh.shape['pcol']

    def local_qr(a_loc, diag_shift):
        rows, ok = gram_rows(a_loc, diag_shift)
        return lax.cond(ok[0, 0] > 0.5, lambda a, s, r: r, lambda a, s, r: householder_rows(a, s, n_pcol), a_loc, diag_shift, rows)

    return jax.shard_map(local_qr, mesh=mesh, in_specs=(P(('batch', 'prow'), 'pcol'), P('batch', None)), out_specs=P('batch', 'pcol'), check_vma=False)
```

```python
import functools

import jax
import jax.numpy as jnp
from jax import lax
from jax.experimental import pallas as pl
from jax.experimental.pallas import tpu as pltpu
from jax.sharding import PartitionSpec as P

PRECISE = lax.Precision.HIGHEST
F32 = jnp.float32
NB = 128
MESH = pl.DeviceIdType.MESH
TRACE_FACTOR = 2.0


def dot_nn(x, y):
    return lax.dot_general(x, y, (((1,), (0,)), ((), ())), precision=PRECISE, preferred_element_type=F32)


def dot_tn(x, y):
    return lax.dot_general(x, y, (((0,), (0,)), ((), ())), precision=PRECISE, preferred_element_type=F32)


def gather_sum(x, axis):
    return jnp.sum(lax.all_gather(x, axis), axis=0)


def factor_panel(panel, glob_rows, col_base):
    blocksize = panel.shape[1]
    lane_ids = jnp.arange(blocksize)

    def col_step(k, loop_state):
        panel, vectors, tau_vec, sign_vec = loop_state
        glob_col = col_base + k
        active = glob_rows >= glob_col
        is_pivot = glob_rows == glob_col
        column = lax.dynamic_slice_in_dim(panel, k, 1, axis=1)[:, 0]
        reduced = gather_sum(jnp.stack([jnp.sum(jnp.where(active, column, 0.0)[:, None] * panel, axis=0),
                                        jnp.sum(jnp.where(is_pivot[:, None], panel, 0.0), axis=0)]), 'prow')
        col_dots = reduced[0]
        pivot_row = reduced[1]
        pivot_val = lax.dynamic_index_in_dim(pivot_row, k, keepdims=False)
        col_norm = jnp.sqrt(lax.dynamic_index_in_dim(col_dots, k, keepdims=False))
        beta_val = jnp.where(pivot_val >= 0, -col_norm, col_norm)
        tau_val = (beta_val - pivot_val) / beta_val
        inv_scale = 1.0 / (pivot_val - beta_val)
        v_col = jnp.where(is_pivot, 1.0, jnp.where(active, column * inv_scale, 0.0))
        v_dots = inv_scale * (col_dots - pivot_val * pivot_row) + pivot_row
        update = jnp.where(lane_ids > k, tau_val * v_dots, 0.0)
        new_col = jnp.where(active, jnp.where(is_pivot, beta_val, 0.0), column)
        panel = panel - v_col[:, None] * update[None, :]
        panel = lax.dynamic_update_slice_in_dim(panel, new_col[:, None], k, axis=1)
        vectors = lax.dynamic_update_slice_in_dim(vectors, v_col[:, None], k, axis=1)
        tau_vec = jnp.where(lane_ids == k, tau_val, tau_vec)
        sign_vec = jnp.where(lane_ids == k, jnp.where(beta_val < 0, -1.0, 1.0), sign_vec)
        return panel, vectors, tau_vec, sign_vec

    init_state = (panel, jnp.zeros_like(panel), jnp.zeros((blocksize,), F32), jnp.zeros((blocksize,), F32))
    return lax.fori_loop(0, blocksize, col_step, init_state)


def build_tfactor(gram_mat, tau_vec):
    blocksize = tau_vec.shape[0]
    lane_ids = jnp.arange(blocksize)

    def t_step(k, t_factor):
        gram_col = jnp.where(lane_ids < k, lax.dynamic_slice_in_dim(gram_mat, k, 1, axis=1)[:, 0], 0.0)
        tau_k = lax.dynamic_index_in_dim(tau_vec, k, keepdims=False)
        column = -tau_k * jnp.sum(t_factor * gram_col[None, :], axis=1)
        column = jnp.where(lane_ids == k, tau_k, column)
        return jnp.where(lane_ids[None, :] == k, column[:, None], t_factor)

    return lax.fori_loop(0, blocksize, t_step, jnp.zeros((blocksize, blocksize), F32))


def householder_rows(a_loc, diag_shift, n_pcol):
    rows_loc, cols_loc = a_loc.shape
    panels, blocksize = diag_shift.shape
    total_k = panels * blocksize
    row_id = lax.axis_index('prow')
    col_id = lax.axis_index('pcol')
    glob_rows = row_id * rows_loc + jnp.arange(rows_loc)
    local_cols = jnp.arange(cols_loc)
    orig_cols = ((local_cols // blocksize) * n_pcol + col_id) * blocksize + local_cols % blocksize
    shift_flat = diag_shift.reshape(total_k)
    col_shift = jnp.where(orig_cols < total_k, shift_flat[jnp.minimum(orig_cols, total_k - 1)], 0.0)
    a_loc = a_loc + jnp.where(glob_rows[:, None] == orig_cols[None, :], col_shift[None, :], 0.0)
    swap = [(0, 1), (1, 0)]

    def owned(x, is_owner):
        return jnp.where(is_owner, x, lax.ppermute(x, 'pcol', swap))

    def panel_step(panel_idx, state):
        a_loc, signs = state
        owner_col = panel_idx % n_pcol
        start_col = (panel_idx // n_pcol) * blocksize
        is_owner = col_id == owner_col
        panel = lax.dynamic_slice_in_dim(a_loc, start_col, blocksize, axis=1)
        factored, vectors, tau_vec, sign_vec = factor_panel(panel, glob_rows, panel_idx * blocksize)
        gram_mat = gather_sum(jnp.einsum('mi,mj->ij', vectors, vectors, precision=PRECISE, preferred_element_type=F32), 'prow')
        t_factor = build_tfactor(gram_mat, tau_vec)
        vectors, t_factor, sign_vec = owned(vectors, is_owner), owned(t_factor, is_owner), owned(sign_vec, is_owner)
        signs = lax.dynamic_update_slice_in_dim(signs, sign_vec, panel_idx * blocksize, axis=0)
        keep_cols = orig_cols >= (panel_idx + 1) * blocksize
        proj = jnp.einsum('mi,mn->in', vectors, a_loc, precision=PRECISE, preferred_element_type=F32)
        quarter = cols_loc // 4
        proj_sum = jnp.concatenate([gather_sum(proj[:, q * quarter:(q + 1) * quarter], 'prow') for q in range(4)], axis=1)
        w_mat = jnp.where(keep_cols[None, :], jnp.einsum('ij,in->jn', t_factor, proj_sum, precision=PRECISE, preferred_element_type=F32), 0.0)
        a_loc = a_loc - jnp.dot(vectors, w_mat, precision=PRECISE, preferred_element_type=F32)
        kept = lax.dynamic_slice_in_dim(a_loc, start_col, blocksize, axis=1)
        a_loc = lax.dynamic_update_slice_in_dim(a_loc, jnp.where(is_owner, factored, kept), start_col, axis=1)
        return a_loc, signs

    a_loc, signs = lax.fori_loop(0, panels, panel_step, (a_loc, jnp.zeros((total_k,), F32)))
    step = total_k // 8

    def top_step(i, top):
        piece = lax.all_gather(lax.dynamic_slice_in_dim(a_loc, i * step, step, axis=0), 'prow')[0]
        return lax.dynamic_update_slice_in_dim(top, piece, i * step, axis=0)

    top_rows = lax.fori_loop(0, 8, top_step, jnp.zeros((total_k, cols_loc), F32))
    return top_rows * signs[:, None]


def factor_block(block, u_ref, m_ref):
    sub = lax.broadcasted_iota(jnp.int32, (8, NB), 0)
    lane = lax.broadcasted_iota(jnp.int32, (8, NB), 1)
    eye = (lax.broadcasted_iota(jnp.int32, (NB, NB), 0) == lax.broadcasted_iota(jnp.int32, (NB, NB), 1)).astype(F32)
    wide = lambda row: jnp.broadcast_to(row, (8, NB))

    def group(tiles, g, state):
        s_tiles, m_tiles = state[:tiles], state[tiles:]
        base = pl.multiple_of(g * 8, 8)
        spread = lambda tile, t: jnp.take_along_axis(tile, jnp.full((8, NB), base + t, jnp.int32), axis=1)
        s_top, m_top = s_tiles[0], m_tiles[0]
        cols = [spread(s_top, t) for t in range(8)]
        dinv = jnp.zeros((8, NB), F32)
        for s in range(8):
            inv_p = 1.0 / wide(cols[s][s:s + 1])
            dinv = jnp.where(sub == s, inv_p, dinv)
            mult = jnp.where(sub > s, cols[s] * inv_p, 0.0)
            for t in range(s + 1, 8):
                cols[t] = cols[t] - mult * wide(cols[t][s:s + 1])
            s_top = s_top - mult * wide(s_top[s:s + 1])
            m_top = m_top - mult * wide(m_top[s:s + 1])
        scale = jnp.sqrt(dinv)
        u_ref[pl.ds(base, 8), :] = jnp.where(lane >= sub + base, s_top * scale, 0.0)
        m_ref[pl.ds(base, 8), :] = m_top * scale
        s_sol, m_sol = s_top * dinv, m_top * dinv
        for s in range(7, 0, -1):
            mult = jnp.where(sub < s, cols[s] * dinv, 0.0)
            s_sol = s_sol - mult * wide(s_sol[s:s + 1])
            m_sol = m_sol - mult * wide(m_sol[s:s + 1])
        s_rows = [wide(s_sol[t:t + 1]) for t in range(8)]
        m_rows = [wide(m_sol[t:t + 1]) for t in range(8)]
        s_new, m_new = [], []
        for v in range(1, tiles):
            s_acc, m_acc = s_tiles[v], m_tiles[v]
            for t in range(8):
                col = spread(s_tiles[v], t)
                s_acc = s_acc - col * s_rows[t]
                m_acc = m_acc - col * m_rows[t]
            s_new.append(s_acc)
            m_new.append(m_acc)
        zero = jnp.zeros((8, NB), F32)
        return tuple(s_new + [zero] + m_new + [zero])

    def tiles_of(x):
        return [x[8 * v:8 * v + 8] for v in range(x.shape[0] // 8)]

    n = NB // 8
    state = tuple(tiles_of(block) + tiles_of(eye))
    done = 0
    for tiles, steps in ((n, n // 2), (n // 2, n // 2)):
        state = lax.fori_loop(done, done + steps, functools.partial(group, tiles), state)
        done += steps
        half = len(state) // 2
        state = state[:n - done] + state[half:half + n - done]


def gram_kernel(a_hbm, s_hbm, r_ref, ok_ref, s_ref, w_buf, y_buf, acc1, acc2, acc1_r, h_buf, cm_buf, cm_recv, cy_recv, cfin,
                xp, xp_r, tail_r, tail_s, last_buf, z_buf, t_buf, rf_buf, k12, ymax, u_blk, m_blk,
                load_sem, ya_send, ya_recv, yb_send, yb_recv, ar_send, ar_recv, gy_send, gy_recv, gq_send, gq_recv,
                rs_send, rs_recv, cy_send, cy_rsem, ag_send, ag_recv, s_sem):
    rows, cols = a_hbm.shape
    half_rows = rows // 2
    half = cols // 2
    kk = 2 * half
    c = lax.axis_index('pcol')
    p = lax.axis_index('prow')
    other = 1 - c
    core_peer = p + 1 - 2 * (p % 2)
    x_peer = (p + 2) % 4
    qr = half // 4
    ca = 512
    n_a = half_rows // ca
    b_cuts = ((0, 768, 1920, 3072), (0, 1024, 2048, 2816, 3072))
    n_b = [len(cuts) - 1 for cuts in b_cuts]
    n_l = rows // ca

    def row0(start, size):
        return pl.ds(pl.multiple_of(start, NB), size)

    def load(j):
        rs = pl.ds(pl.multiple_of(j * ca, ca), ca)
        return (pltpu.make_async_copy(a_hbm.at[rs, pl.ds(0, half)], w_buf.at[c, rs, :], load_sem.at[0, j]),
                pltpu.make_async_copy(a_hbm.at[rs, pl.ds(half, half)], y_buf.at[rs, :], load_sem.at[1, j]))

    barrier = pltpu.get_barrier_semaphore()
    pl.semaphore_signal(barrier, inc=1, device_id={'pcol': other}, device_id_type=MESH)
    for d in range(1, 4):
        pl.semaphore_signal(barrier, inc=1, device_id={'prow': (p + d) % 4}, device_id_type=MESH)
    s_load = pltpu.make_async_copy(s_hbm, s_ref, s_sem)
    s_load.start()
    for j in range(n_l):
        for cp in load(j):
            cp.start()
    pl.semaphore_wait(barrier, 4)

    def send_a(k):
        rs = row0(c * half_rows + k * ca, ca)
        return pltpu.make_async_remote_copy(a_hbm.at[rs, pl.ds(0, half)], w_buf.at[c, rs, :], ya_send.at[k], ya_recv.at[k],
                                            device_id={'pcol': other}, device_id_type=MESH)

    def send_b(l, k):
        rs = row0(other * half_rows + b_cuts[l][k], b_cuts[l][k + 1] - b_cuts[l][k])
        ls = pl.ds(l * NB, NB)
        return pltpu.make_async_remote_copy(a_hbm.at[rs, ls], w_buf.at[c, rs, ls], yb_send.at[l, k], yb_recv.at[l, k],
                                            device_id={'pcol': other}, device_id_type=MESH)

    for k in range(4):
        send_a(k).start()

    eye = (lax.broadcasted_iota(jnp.int32, (NB, NB), 0) == lax.broadcasted_iota(jnp.int32, (NB, NB), 1)).astype(F32)

    def add_shift(side, l, cond):
        @pl.when(jnp.logical_and(p == 0, cond))
        def _():
            panel = 2 * l + side
            rs = row0(panel * NB, NB)
            w_buf[side, rs, l * NB:(l + 1) * NB] = w_buf[side, rs, l * NB:(l + 1) * NB] + eye * s_ref[pl.ds(panel, 1), :]

    acc1[...] = jnp.zeros_like(acc1)
    acc2[...] = jnp.zeros_like(acc2)
    ymax[...] = jnp.zeros_like(ymax)
    s_load.wait()

    @pl.loop(0, n_l)
    def _(j):
        for cp in load(j):
            cp.wait()
        for l in range(2):
            add_shift(c, l, j == 0)
        rs = pl.ds(pl.multiple_of(j * ca, ca), ca)
        left = w_buf[c, rs, :]
        right = y_buf[rs, :]
        ymax[...] = jnp.maximum(ymax[...], jnp.max(jnp.abs(right).reshape(ca // 8, 8, half), axis=0))
        acc1[...] += dot_tn(left, jnp.concatenate([left, right], axis=1))

    def pair_copy(src, dst, slot, peer):
        return pltpu.make_async_remote_copy(src, dst, ar_send.at[slot], ar_recv.at[slot], device_id={'prow': peer}, device_id_type=MESH)

    g1 = pair_copy(acc1, acc1_r.at[0], 0, core_peer)
    g1.start()
    g1.wait()
    acc1[...] += acc1_r[0]
    g2 = pair_copy(acc1, acc1_r.at[1], 1, x_peer)
    g2.start()
    g2.wait()
    acc1[...] += acc1_r[1]
    h_buf[c] = acc1[:, :half]
    quarter = pl.ds(pl.multiple_of(p * qr, qr), qr)
    gy = pltpu.make_async_remote_copy(h_buf.at[c, quarter, :], h_buf.at[c, quarter, :], gy_send, gy_recv,
                                      device_id={'pcol': other}, device_id_type=MESH)
    gy.start()
    for k in range(4, n_a):
        send_a(k).start()
    send_b(0, 0).start()

    def take_a(k):
        send_a(k).wait_recv()
        for l in range(2):
            add_shift(other, l, jnp.logical_and(c == 1, k == 0))
        rs = row0(other * half_rows + k * ca, ca)
        right = jnp.concatenate([w_buf[c, rs, :], y_buf[rs, :]], axis=1)
        acc2[...] += dot_tn(w_buf[other, rs, :], right)

    def spread_gram(d, src):
        rs = pl.ds(pl.multiple_of(src * qr, qr), qr)
        return pltpu.make_async_remote_copy(h_buf.at[other, rs, :], h_buf.at[other, rs, :], gq_send.at[d], gq_recv.at[d],
                                            device_id={'prow': (p + d) % 4}, device_id_type=MESH)

    @pl.loop(0, n_a)
    def _(k):
        take_a(k)

        @pl.when(k == n_a - 3)
        def _():
            gy.wait()
            for d in range(1, 4):
                spread_gram(d, p).start()

        @pl.when(k == n_a - 2)
        def _():
            for d in range(1, 4):
                spread_gram(d, p).wait_send()
                spread_gram(d, (p + 4 - d) % 4).wait_recv()
            factor_block(h_buf[0, :NB, :NB], u_blk, m_blk)

    @pl.when(c == 0)
    def _():
        ct = acc2[:, :half].T
        for q in range(4):
            cm_buf[q, :qr, :] = ct[q * qr:(q + 1) * qr]

    @pl.when(c == 1)
    def _():
        for q in range(4):
            cm_buf[q, :qr, :] = acc2[q * qr:(q + 1) * qr, :half]

    for q in range(4):
        cm_buf[q, qr:, :] = ymax[...]

    def scatter(d):
        q = (p + d) % 4
        return pltpu.make_async_remote_copy(cm_buf.at[q], cm_recv.at[d - 1], rs_send.at[d], rs_recv.at[d],
                                            device_id={'prow': q}, device_id_type=MESH)

    for d in range(1, 4):
        scatter(d).start()
    for l in range(2):
        xp[l] = acc2[l * NB:(l + 1) * NB, half:]
    for d in range(1, 4):
        scatter(d).wait()
    cm_buf[p] = ((cm_buf[p] + cm_recv[0]) + cm_recv[1]) + cm_recv[2]
    cy = pltpu.make_async_remote_copy(cm_buf.at[p], cy_recv, cy_send, cy_rsem, device_id={'pcol': other}, device_id_type=MESH)
    cy.start()
    for k in range(1, n_b[0]):
        send_b(0, k).start()
    for k in range(n_b[1]):
        send_b(1, k).start()
    cy.wait()
    cfin[p] = cm_buf[p] + cy_recv[...]

    def spread(d, src):
        return pltpu.make_async_remote_copy(cfin.at[src], cfin.at[src], ag_send.at[d], ag_recv.at[d],
                                            device_id={'prow': (p + d) % 4}, device_id_type=MESH)

    for d in range(1, 4):
        spread(d, p).start()

    for d in range(1, 4):
        spread(d, p).wait_send()
        spread(d, (p + 4 - d) % 4).wait_recv()

    cross = jnp.concatenate([cfin[q, :qr, :] for q in range(4)], axis=0)
    z_buf[...] = jnp.zeros_like(z_buf)
    diag_max = jnp.zeros((1, NB), F32)
    diag_min = jnp.full((1, NB), jnp.inf, F32)
    diags = []
    for i in range(4):
        ci, li = i % 2, i // 2
        for j in range(i, 4):
            cj, lj = j % 2, j // 2
            if ci == cj:
                block = h_buf[ci, li * NB:(li + 1) * NB, lj * NB:(lj + 1) * NB]
            elif ci == 0:
                block = cross[li * NB:(li + 1) * NB, lj * NB:(lj + 1) * NB]
            else:
                block = cross[lj * NB:(lj + 1) * NB, li * NB:(li + 1) * NB].T
            z_buf[i * NB:(i + 1) * NB, j * NB:(j + 1) * NB] = block
            if i == j:
                d_row = jnp.sum(block * eye, axis=0, keepdims=True)
                diags.append(d_row)
                diag_max = jnp.maximum(diag_max, d_row)
                diag_min = jnp.minimum(diag_min, d_row)

    t_buf[...] = jnp.zeros_like(t_buf)
    rf_buf[...] = jnp.zeros_like(rf_buf)
    for j in range(4):
        lo, hi = j * NB, (j + 1) * NB
        if j > 0:
            factor_block(z_buf[lo:hi, lo:hi], u_blk, m_blk)
        inv_t = m_blk[...]
        rf_buf[lo:hi, lo:hi] = u_blk[...]
        t_buf[lo:hi, lo:hi] = inv_t
        new_row = dot_nn(inv_t, z_buf[lo:hi, :])
        if j > 0:
            t_buf[lo:hi, :lo] = new_row[:, :lo]
        if j < 3:
            rf_buf[lo:hi, hi:] = new_row[:, hi:]
            parts = ([new_row[:, :lo]] if j > 0 else []) + [inv_t, new_row[:, hi:]]
            mult = jnp.concatenate(parts, axis=1)
            z_buf[hi:, lo:hi] = jnp.zeros((kk - hi, NB), F32)
            z_buf[hi:, :] = z_buf[hi:, :] - dot_tn(new_row[:, hi:], mult)

    trace = jnp.zeros((1, NB), F32)
    for i in range(4):
        tc = t_buf[i * NB:, i * NB:(i + 1) * NB]
        trace = trace + jnp.sum(tc * tc, axis=0, keepdims=True) * diags[i]
    total = jnp.sum(trace, axis=1, keepdims=True)
    d_max = jnp.max(diag_max, axis=1, keepdims=True)
    d_min = jnp.min(diag_min, axis=1, keepdims=True)
    y_max = jnp.max(jnp.max(cfin[0, qr:, :], axis=0, keepdims=True), axis=1, keepdims=True)
    good = (total < TRACE_FACTOR * kk) & (d_min > 1e-26) & (d_max < 1e36) & (y_max * jnp.sqrt(d_max) < 1e33)
    ok_ref[0, 0] = jnp.where(good, 1, 0)[0, 0]

    for l in range(2):
        ls = pl.ds(pl.multiple_of((2 * l + c) * NB, NB), NB)
        r_ref[:, l * NB:(l + 1) * NB] = rf_buf[:, ls]

    k12[row0(c * NB, NB), :] = acc1[:NB, half:]
    k12[row0((c + 2) * NB, NB), :] = acc1[NB:, half:]
    k12[row0((3 - c) * NB, NB), :] = jnp.zeros((NB, half), F32)

    def take_b(l, k):
        send_b(l, k).wait_recv()
        if k == 0:
            add_shift(other, l, c == 0)
        rs = row0(c * half_rows + b_cuts[l][k], b_cuts[l][k + 1] - b_cuts[l][k])
        xp[l] += dot_tn(w_buf[other, rs, l * NB:(l + 1) * NB], y_buf[rs, :])

    for k in range(n_b[0]):
        take_b(0, k)
    x1 = pair_copy(xp.at[0], xp_r.at[0], 2, core_peer)
    x1.start()
    x1.wait()
    xp[0] = xp[0] + xp_r[0]
    x2 = pair_copy(xp.at[0], xp_r.at[1], 3, x_peer)
    x2.start()
    x2.wait()
    k12[row0((1 - c) * NB, NB), :] = xp[0] + xp_r[1]
    r_ref[:, half:] = dot_nn(t_buf[...], k12[...])
    for k in range(n_b[1]):
        take_b(1, k)
    mine = pl.ds(pl.multiple_of((p % 2) * (NB // 2), NB // 2), NB // 2)
    theirs = pl.ds(pl.multiple_of((1 - p % 2) * (NB // 2), NB // 2), NB // 2)
    x3 = pair_copy(xp.at[1, theirs, :], tail_r.at[0], 4, core_peer)
    x3.start()
    x3.wait()
    tail_s[...] = xp[1, mine, :] + tail_r[0]
    x4 = pair_copy(tail_s, tail_r.at[1], 5, x_peer)
    x4.start()
    x4.wait()
    last_buf[mine, :] = tail_s[...] + tail_r[1]
    x5 = pair_copy(last_buf.at[mine, :], last_buf.at[mine, :], 6, core_peer)
    x5.start()
    x5.wait()
    r_ref[half:, half:] += dot_nn(t_buf[half:, pl.ds(pl.multiple_of((3 - c) * NB, NB), NB)], last_buf[...])

    for k in range(n_a):
        send_a(k).wait_send()
    for l in range(2):
        for k in range(n_b[l]):
            send_b(l, k).wait_send()


def gram_rows(a_loc, diag_shift):
    rows, cols = a_loc.shape
    half = cols // 2
    kk = cols
    qr = half // 4
    dma = pltpu.SemaphoreType.DMA
    vm = lambda *shape: pltpu.VMEM(shape, F32)
    return pl.pallas_call(
        gram_kernel,
        out_shape=(pltpu.VMEM((kk, cols), F32), pltpu.SMEM((1, 1), jnp.int32)),
        in_specs=[pl.BlockSpec(memory_space=pl.ANY), pl.BlockSpec(memory_space=pl.ANY)],
        out_specs=(pl.BlockSpec(memory_space=pltpu.VMEM), pl.BlockSpec(memory_space=pltpu.SMEM)),
        scratch_shapes=[
            vm(*diag_shift.shape),
            vm(2, rows, half), vm(rows, half), vm(half, cols), vm(half, cols), vm(2, half, cols), vm(2, half, half),
            vm(4, qr + 8, half), vm(3, qr + 8, half), vm(qr + 8, half), vm(4, qr + 8, half),
            vm(2, NB, half), vm(2, NB, half), vm(2, NB // 2, half), vm(NB // 2, half), vm(NB, half), vm(kk, kk), vm(kk, kk), vm(kk, kk), vm(kk, half), vm(8, half),
            vm(NB, NB), vm(NB, NB),
            dma((2, rows // 512)), dma((rows // 1024,)), dma((rows // 1024,)), dma((2, 4)), dma((2, 4)),
            dma((7,)), dma((7,)), dma, dma, dma((4,)), dma((4,)),
            dma((4,)), dma((4,)), dma, dma, dma((4,)), dma((4,)), dma,
        ],
        compiler_params=pltpu.CompilerParams(collective_id=0, has_side_effects=True, vmem_limit_bytes=48 * 1024 * 1024),
        name='gram_rows',
    )(a_loc, diag_shift)


def solution(mesh):
    n_pcol = mesh.shape['pcol']

    def local_qr(a_loc, diag_shift):
        rows, ok = gram_rows(a_loc, diag_shift)
        return lax.cond(ok[0, 0] != 0, lambda a, s, r: r, lambda a, s, r: householder_rows(a, s, n_pcol), a_loc, diag_shift, rows)

    return jax.shard_map(local_qr, mesh=mesh, in_specs=(P(('batch', 'prow'), 'pcol'), P('batch', None)), out_specs=P('batch', 'pcol'), check_vma=False)
```

```python
import functools

import jax
import jax.numpy as jnp
from jax import lax
from jax.experimental import pallas as pl
from jax.experimental.pallas import tpu as pltpu
from jax.sharding import PartitionSpec as P

PRECISE = lax.Precision.HIGHEST
F32 = jnp.float32
NB = 128
MESH = pl.DeviceIdType.MESH
TRACE_FACTOR = 2.0


def dot_nn(x, y):
    return lax.dot_general(x, y, (((1,), (0,)), ((), ())), precision=PRECISE, preferred_element_type=F32)


def dot_tn(x, y):
    return lax.dot_general(x, y, (((0,), (0,)), ((), ())), precision=PRECISE, preferred_element_type=F32)


def gather_sum(x, axis):
    return jnp.sum(lax.all_gather(x, axis), axis=0)


def factor_panel(panel, glob_rows, col_base):
    blocksize = panel.shape[1]
    lane_ids = jnp.arange(blocksize)

    def col_step(k, loop_state):
        panel, vectors, tau_vec, sign_vec = loop_state
        glob_col = col_base + k
        active = glob_rows >= glob_col
        is_pivot = glob_rows == glob_col
        column = lax.dynamic_slice_in_dim(panel, k, 1, axis=1)[:, 0]
        reduced = gather_sum(jnp.stack([jnp.sum(jnp.where(active, column, 0.0)[:, None] * panel, axis=0),
                                        jnp.sum(jnp.where(is_pivot[:, None], panel, 0.0), axis=0)]), 'prow')
        col_dots = reduced[0]
        pivot_row = reduced[1]
        pivot_val = lax.dynamic_index_in_dim(pivot_row, k, keepdims=False)
        col_norm = jnp.sqrt(lax.dynamic_index_in_dim(col_dots, k, keepdims=False))
        beta_val = jnp.where(pivot_val >= 0, -col_norm, col_norm)
        tau_val = (beta_val - pivot_val) / beta_val
        inv_scale = 1.0 / (pivot_val - beta_val)
        v_col = jnp.where(is_pivot, 1.0, jnp.where(active, column * inv_scale, 0.0))
        v_dots = inv_scale * (col_dots - pivot_val * pivot_row) + pivot_row
        update = jnp.where(lane_ids > k, tau_val * v_dots, 0.0)
        new_col = jnp.where(active, jnp.where(is_pivot, beta_val, 0.0), column)
        panel = panel - v_col[:, None] * update[None, :]
        panel = lax.dynamic_update_slice_in_dim(panel, new_col[:, None], k, axis=1)
        vectors = lax.dynamic_update_slice_in_dim(vectors, v_col[:, None], k, axis=1)
        tau_vec = jnp.where(lane_ids == k, tau_val, tau_vec)
        sign_vec = jnp.where(lane_ids == k, jnp.where(beta_val < 0, -1.0, 1.0), sign_vec)
        return panel, vectors, tau_vec, sign_vec

    init_state = (panel, jnp.zeros_like(panel), jnp.zeros((blocksize,), F32), jnp.zeros((blocksize,), F32))
    return lax.fori_loop(0, blocksize, col_step, init_state)


def build_tfactor(gram_mat, tau_vec):
    blocksize = tau_vec.shape[0]
    lane_ids = jnp.arange(blocksize)

    def t_step(k, t_factor):
        gram_col = jnp.where(lane_ids < k, lax.dynamic_slice_in_dim(gram_mat, k, 1, axis=1)[:, 0], 0.0)
        tau_k = lax.dynamic_index_in_dim(tau_vec, k, keepdims=False)
        column = -tau_k * jnp.sum(t_factor * gram_col[None, :], axis=1)
        column = jnp.where(lane_ids == k, tau_k, column)
        return jnp.where(lane_ids[None, :] == k, column[:, None], t_factor)

    return lax.fori_loop(0, blocksize, t_step, jnp.zeros((blocksize, blocksize), F32))


def householder_rows(a_loc, diag_shift, n_pcol):
    rows_loc, cols_loc = a_loc.shape
    panels, blocksize = diag_shift.shape
    total_k = panels * blocksize
    row_id = lax.axis_index('prow')
    col_id = lax.axis_index('pcol')
    glob_rows = row_id * rows_loc + jnp.arange(rows_loc)
    local_cols = jnp.arange(cols_loc)
    orig_cols = ((local_cols // blocksize) * n_pcol + col_id) * blocksize + local_cols % blocksize
    shift_flat = diag_shift.reshape(total_k)
    col_shift = jnp.where(orig_cols < total_k, shift_flat[jnp.minimum(orig_cols, total_k - 1)], 0.0)
    a_loc = a_loc + jnp.where(glob_rows[:, None] == orig_cols[None, :], col_shift[None, :], 0.0)
    swap = [(0, 1), (1, 0)]

    def owned(x, is_owner):
        return jnp.where(is_owner, x, lax.ppermute(x, 'pcol', swap))

    def panel_step(panel_idx, state):
        a_loc, signs = state
        owner_col = panel_idx % n_pcol
        start_col = (panel_idx // n_pcol) * blocksize
        is_owner = col_id == owner_col
        panel = lax.dynamic_slice_in_dim(a_loc, start_col, blocksize, axis=1)
        factored, vectors, tau_vec, sign_vec = factor_panel(panel, glob_rows, panel_idx * blocksize)
        gram_mat = gather_sum(jnp.einsum('mi,mj->ij', vectors, vectors, precision=PRECISE, preferred_element_type=F32), 'prow')
        t_factor = build_tfactor(gram_mat, tau_vec)
        vectors, t_factor, sign_vec = owned(vectors, is_owner), owned(t_factor, is_owner), owned(sign_vec, is_owner)
        signs = lax.dynamic_update_slice_in_dim(signs, sign_vec, panel_idx * blocksize, axis=0)
        keep_cols = orig_cols >= (panel_idx + 1) * blocksize
        proj = jnp.einsum('mi,mn->in', vectors, a_loc, precision=PRECISE, preferred_element_type=F32)
        quarter = cols_loc // 4
        proj_sum = jnp.concatenate([gather_sum(proj[:, q * quarter:(q + 1) * quarter], 'prow') for q in range(4)], axis=1)
        w_mat = jnp.where(keep_cols[None, :], jnp.einsum('ij,in->jn', t_factor, proj_sum, precision=PRECISE, preferred_element_type=F32), 0.0)
        a_loc = a_loc - jnp.dot(vectors, w_mat, precision=PRECISE, preferred_element_type=F32)
        kept = lax.dynamic_slice_in_dim(a_loc, start_col, blocksize, axis=1)
        a_loc = lax.dynamic_update_slice_in_dim(a_loc, jnp.where(is_owner, factored, kept), start_col, axis=1)
        return a_loc, signs

    a_loc, signs = lax.fori_loop(0, panels, panel_step, (a_loc, jnp.zeros((total_k,), F32)))
    step = total_k // 8

    def top_step(i, top):
        piece = lax.all_gather(lax.dynamic_slice_in_dim(a_loc, i * step, step, axis=0), 'prow')[0]
        return lax.dynamic_update_slice_in_dim(top, piece, i * step, axis=0)

    top_rows = lax.fori_loop(0, 8, top_step, jnp.zeros((total_k, cols_loc), F32))
    return top_rows * signs[:, None]


def factor_block(block, u_ref, m_ref):
    sub = lax.broadcasted_iota(jnp.int32, (8, NB), 0)
    lane = lax.broadcasted_iota(jnp.int32, (8, NB), 1)
    eye = (lax.broadcasted_iota(jnp.int32, (NB, NB), 0) == lax.broadcasted_iota(jnp.int32, (NB, NB), 1)).astype(F32)
    wide = lambda row: jnp.broadcast_to(row, (8, NB))

    def group(tiles, g, state):
        s_tiles, m_tiles = state[:tiles], state[tiles:]
        base = pl.multiple_of(g * 8, 8)
        spread = lambda tile, t: jnp.take_along_axis(tile, jnp.full((8, NB), base + t, jnp.int32), axis=1)
        s_top, m_top = s_tiles[0], m_tiles[0]
        cols = [spread(s_top, t) for t in range(8)]
        dinv = jnp.zeros((8, NB), F32)
        for s in range(8):
            inv_p = 1.0 / wide(cols[s][s:s + 1])
            dinv = jnp.where(sub == s, inv_p, dinv)
            mult = jnp.where(sub > s, cols[s] * inv_p, 0.0)
            for t in range(s + 1, 8):
                cols[t] = cols[t] - mult * wide(cols[t][s:s + 1])
            s_top = s_top - mult * wide(s_top[s:s + 1])
            m_top = m_top - mult * wide(m_top[s:s + 1])
        scale = jnp.sqrt(dinv)
        u_ref[pl.ds(base, 8), :] = jnp.where(lane >= sub + base, s_top * scale, 0.0)
        m_ref[pl.ds(base, 8), :] = m_top * scale
        s_sol, m_sol = s_top * dinv, m_top * dinv
        for s in range(7, 0, -1):
            mult = jnp.where(sub < s, cols[s] * dinv, 0.0)
            s_sol = s_sol - mult * wide(s_sol[s:s + 1])
            m_sol = m_sol - mult * wide(m_sol[s:s + 1])
        s_rows = [wide(s_sol[t:t + 1]) for t in range(8)]
        m_rows = [wide(m_sol[t:t + 1]) for t in range(8)]
        s_new, m_new = [], []
        for v in range(1, tiles):
            s_acc, m_acc = s_tiles[v], m_tiles[v]
            for t in range(8):
                col = spread(s_tiles[v], t)
                s_acc = s_acc - col * s_rows[t]
                m_acc = m_acc - col * m_rows[t]
            s_new.append(s_acc)
            m_new.append(m_acc)
        zero = jnp.zeros((8, NB), F32)
        return tuple(s_new + [zero] + m_new + [zero])

    def tiles_of(x):
        return [x[8 * v:8 * v + 8] for v in range(x.shape[0] // 8)]

    n = NB // 8
    state = tuple(tiles_of(block) + tiles_of(eye))
    done = 0
    for tiles, steps in ((n, n // 2), (n // 2, n // 2)):
        state = lax.fori_loop(done, done + steps, functools.partial(group, tiles), state)
        done += steps
        half = len(state) // 2
        state = state[:n - done] + state[half:half + n - done]


def gram_kernel(a_hbm, s_hbm, r_ref, ok_ref, s_ref, own, peer, acc1, acc2, acc1_r, hb, cm_buf, cm_recv, cy_recv, cfin,
                xp, xp_r, tail_r, tail_s, done_s, done_r, z_buf, t_buf, rf_buf, k12, ymax, u_blk, m_blk,
                load_sem, ya_send, ya_recv, yb_send, yb_recv, ar_send, ar_recv, gy_send, gy_recv, gq_send, gq_recv,
                rs_send, rs_recv, cy_send, cy_rsem, ag_send, ag_recv, s_sem):
    rows, cols = a_hbm.shape
    half_rows = rows // 2
    half = cols // 2
    kk = 2 * half
    c = lax.axis_index('pcol')
    p = lax.axis_index('prow')
    other = 1 - c
    core = p % 2
    core_peer = p + 1 - 2 * core
    x_peer = (p + 2) % 4
    qr = half // 4
    qb = NB // 4
    ca = 512
    n_a = half_rows // ca
    n_l = rows // ca
    per_load = n_l // 4
    b_cuts = ((0, 768, 1920, 3072), (0, 1024, 2048, 2944, 3072))
    n_b = [len(cuts) - 1 for cuts in b_cuts]

    def row0(start, size):
        return pl.ds(pl.multiple_of(start, NB), size)

    def to_prow(src, dst, send, recv, q):
        return pltpu.make_async_remote_copy(src, dst, send, recv, device_id={'prow': q}, device_id_type=MESH)

    def to_pcol(src, dst, send, recv):
        return pltpu.make_async_remote_copy(src, dst, send, recv, device_id={'pcol': other}, device_id_type=MESH)

    def load(g):
        rs = row0(g * per_load * ca, per_load * ca)
        return pltpu.make_async_copy(a_hbm.at[rs, :], own.at[rs, :], load_sem.at[g])

    barrier = pltpu.get_barrier_semaphore()
    pl.semaphore_signal(barrier, inc=1, device_id={'pcol': other}, device_id_type=MESH)
    for d in range(1, 4):
        pl.semaphore_signal(barrier, inc=1, device_id={'prow': (p + d) % 4}, device_id_type=MESH)
    s_load = pltpu.make_async_copy(s_hbm, s_ref, s_sem)
    s_load.start()
    for g in range(4):
        load(g).start()
    pl.semaphore_wait(barrier, 4)

    def send_rows(start, size, lanes, send, recv):
        rs = row0(start, size)
        return to_pcol(a_hbm.at[rs, lanes], peer.at[rs, lanes], send, recv)

    def send_a(k):
        return send_rows(c * half_rows + k * ca, ca, pl.ds(0, half), ya_send, ya_recv.at[k])

    def send_b(l, k):
        lo, hi = b_cuts[l][k], b_cuts[l][k + 1]
        return send_rows(other * half_rows + lo, hi - lo, pl.ds(l * NB, NB), yb_send.at[l], yb_recv.at[l, k])

    for k in range(4):
        send_a(k).start()

    eye = (lax.broadcasted_iota(jnp.int32, (NB, NB), 0) == lax.broadcasted_iota(jnp.int32, (NB, NB), 1)).astype(F32)

    def add_shift(ref, side, l, cond):
        @pl.when(jnp.logical_and(p == 0, cond))
        def _():
            panel = 2 * l + side
            rs = row0(panel * NB, NB)
            ref[rs, l * NB:(l + 1) * NB] = ref[rs, l * NB:(l + 1) * NB] + eye * s_ref[pl.ds(panel, 1), :]

    acc1[...] = jnp.zeros_like(acc1)
    acc2[...] = jnp.zeros_like(acc2)
    ymax[...] = jnp.zeros_like(ymax)
    s_load.wait()

    @pl.loop(0, n_l)
    def _(j):
        @pl.when(j % per_load == 0)
        def _():
            load(j // per_load).wait()

        for l in range(2):
            add_shift(own, c, l, j == 0)
        rs = pl.ds(pl.multiple_of(j * ca, ca), ca)
        right = own[rs, :]
        ymax[...] = jnp.maximum(ymax[...], jnp.max(jnp.abs(right[:, half:]).reshape(ca // 8, 8, half), axis=0))
        acc1[...] += dot_tn(right[:, :half], right)

    acc1[NB:NB + 8, :NB] = jnp.maximum(ymax[:, :NB], ymax[:, NB:])

    def pair_copy(src, dst, slot, q):
        return to_prow(src, dst, ar_send.at[slot], ar_recv.at[slot], q)

    g1 = pair_copy(acc1, acc1_r.at[0], 0, core_peer)
    g1.start()
    g1.wait()
    acc1[...] += acc1_r[0]
    g2 = pair_copy(acc1, acc1_r.at[1], 1, x_peer)
    g2.start()
    g2.wait()
    acc1[...] += acc1_r[1]
    for q in range(4):
        rs = slice(q * qb, (q + 1) * qb)
        hb[c, q, :qb, :] = acc1[rs, :NB]
        hb[c, q, qb:2 * qb, :] = acc1[rs, NB:half]
        hb[c, q, 2 * qb:3 * qb, :] = acc1[NB + q * qb:NB + (q + 1) * qb, NB:half]
        hb[c, q, 3 * qb:, :] = acc1[NB:NB + 8, :NB]
    gy = to_pcol(hb.at[c, p], hb.at[c, p], gy_send, gy_recv)
    gy.start()
    for k in range(4, n_a):
        send_a(k).start()
    send_b(0, 0).start()

    def gram_block(side, b):
        return jnp.concatenate([hb[side, q, b * qb:(b + 1) * qb, :] for q in range(4)], axis=0)

    def take_a(k):
        send_a(k).wait_recv()
        for l in range(2):
            add_shift(peer, other, l, jnp.logical_and(c == 1, k == 0))
        rs = row0(other * half_rows + k * ca, ca)
        acc2[...] += dot_tn(peer[rs, :], own[rs, :])

    def spread_gram(d, src):
        return to_prow(hb.at[other, src], hb.at[other, src], gq_send.at[d - 1], gq_recv.at[d - 1], (p + d) % 4)

    @pl.loop(0, n_a)
    def _(k):
        take_a(k)

        @pl.when(k == n_a - 3)
        def _():
            gy.wait()
            for d in range(1, 4):
                spread_gram(d, p).start()

        @pl.when(k == n_a - 2)
        def _():
            for d in range(1, 4):
                spread_gram(d, p).wait_send()
                spread_gram(d, (p + 4 - d) % 4).wait_recv()
            factor_block(gram_block(0, 0), u_blk, m_blk)

    @pl.when(c == 0)
    def _():
        ct = acc2[:, :half].T
        for q in range(4):
            cm_buf[q] = ct[q * qr:(q + 1) * qr]

    @pl.when(c == 1)
    def _():
        for q in range(4):
            cm_buf[q] = acc2[q * qr:(q + 1) * qr, :half]

    def scatter(d):
        q = (p + d) % 4
        return to_prow(cm_buf.at[q], cm_recv.at[d - 1], rs_send.at[d - 1], rs_recv.at[d - 1], q)

    for d in range(1, 4):
        scatter(d).start()
    for l in range(2):
        xp[l] = acc2[l * NB:(l + 1) * NB, half:]
    for d in range(1, 4):
        scatter(d).wait()
    cm_buf[p] = ((cm_buf[p] + cm_recv[0]) + cm_recv[1]) + cm_recv[2]
    cy = to_pcol(cm_buf.at[p], cy_recv, cy_send, cy_rsem)
    cy.start()
    for k in range(1, n_b[0]):
        send_b(0, k).start()
    for k in range(n_b[1]):
        send_b(1, k).start()
    cy.wait()
    cfin[p] = cm_buf[p] + cy_recv[...]

    def spread(d, src):
        return to_prow(cfin.at[src], cfin.at[src], ag_send.at[d - 1], ag_recv.at[d - 1], (p + d) % 4)

    for d in range(1, 4):
        spread(d, p).start()
    for d in range(1, 4):
        spread(d, p).wait_send()
        spread(d, (p + 4 - d) % 4).wait_recv()

    cross = jnp.concatenate([cfin[q] for q in range(4)], axis=0)
    z_buf[...] = jnp.zeros_like(z_buf)
    diag_max = jnp.zeros((1, NB), F32)
    diag_min = jnp.full((1, NB), jnp.inf, F32)
    diags = []
    for i in range(4):
        ci, li = i % 2, i // 2
        for j in range(i, 4):
            cj, lj = j % 2, j // 2
            if ci == cj:
                block = gram_block(ci, li + lj)
            elif ci == 0:
                block = cross[li * NB:(li + 1) * NB, lj * NB:(lj + 1) * NB]
            else:
                block = cross[lj * NB:(lj + 1) * NB, li * NB:(li + 1) * NB].T
            z_buf[i * NB:(i + 1) * NB, j * NB:(j + 1) * NB] = block
            if i == j:
                d_row = jnp.sum(block * eye, axis=0, keepdims=True)
                diags.append(d_row)
                diag_max = jnp.maximum(diag_max, d_row)
                diag_min = jnp.minimum(diag_min, d_row)

    t_buf[...] = jnp.zeros_like(t_buf)
    rf_buf[...] = jnp.zeros_like(rf_buf)
    for j in range(4):
        lo, hi = j * NB, (j + 1) * NB
        if j > 0:
            factor_block(z_buf[lo:hi, lo:hi], u_blk, m_blk)
        inv_t = m_blk[...]
        rf_buf[lo:hi, lo:hi] = u_blk[...]
        t_buf[lo:hi, lo:hi] = inv_t
        new_row = dot_nn(inv_t, z_buf[lo:hi, :])
        if j > 0:
            t_buf[lo:hi, :lo] = new_row[:, :lo]
        if j < 3:
            rf_buf[lo:hi, hi:] = new_row[:, hi:]
            parts = ([new_row[:, :lo]] if j > 0 else []) + [inv_t, new_row[:, hi:]]
            mult = jnp.concatenate(parts, axis=1)
            z_buf[hi:, lo:hi] = jnp.zeros((kk - hi, NB), F32)
            z_buf[hi:, :] = z_buf[hi:, :] - dot_tn(new_row[:, hi:], mult)

    trace = jnp.zeros((1, NB), F32)
    for i in range(4):
        tc = t_buf[i * NB:, i * NB:(i + 1) * NB]
        trace = trace + jnp.sum(tc * tc, axis=0, keepdims=True) * diags[i]
    total = jnp.sum(trace, axis=1, keepdims=True)
    d_max = jnp.max(diag_max, axis=1, keepdims=True)
    d_min = jnp.min(diag_min, axis=1, keepdims=True)
    y_max = jnp.maximum(hb[0, 0, 3 * qb:, :], hb[1, 0, 3 * qb:, :])
    y_max = jnp.max(jnp.max(y_max, axis=0, keepdims=True), axis=1, keepdims=True)
    good = (total < TRACE_FACTOR * kk) & (d_min > 1e-26) & (d_max < 1e36) & (y_max * jnp.sqrt(d_max) < 1e33)
    ok_ref[0, 0] = jnp.where(good, 1, 0)[0, 0]

    for l in range(2):
        ls = pl.ds(pl.multiple_of((2 * l + c) * NB, NB), NB)
        r_ref[:, l * NB:(l + 1) * NB] = rf_buf[:, ls]

    k12[row0(c * NB, NB), :] = acc1[:NB, half:]
    k12[row0((c + 2) * NB, NB), :] = acc1[NB:, half:]
    k12[row0((3 - c) * NB, NB), :] = jnp.zeros((NB, half), F32)

    def take_b(l, k):
        send_b(l, k).wait_recv()
        if k == 0:
            add_shift(peer, other, l, c == 0)
        rs = row0(c * half_rows + b_cuts[l][k], b_cuts[l][k + 1] - b_cuts[l][k])
        xp[l] += dot_tn(peer[rs, l * NB:(l + 1) * NB], own[rs, half:])

    for k in range(n_b[0]):
        take_b(0, k)
    x1 = pair_copy(xp.at[0], xp_r.at[0], 2, core_peer)
    x1.start()
    x1.wait()
    xp[0] = xp[0] + xp_r[0]
    x2 = pair_copy(xp.at[0], xp_r.at[1], 3, x_peer)
    x2.start()
    x2.wait()
    k12[row0((1 - c) * NB, NB), :] = xp[0] + xp_r[1]
    r_ref[:, half:] = dot_nn(t_buf[...], k12[...])
    for k in range(n_b[1]):
        take_b(1, k)
    mine = pl.ds(pl.multiple_of(core * NB, NB), NB)
    theirs = pl.ds(pl.multiple_of((1 - core) * NB, NB), NB)
    x3 = pair_copy(xp.at[1, :, theirs], tail_r.at[0], 4, core_peer)
    x3.start()
    x3.wait()
    tail_s[...] = xp[1, :, mine] + tail_r[0]
    x4 = pair_copy(tail_s, tail_r.at[1], 5, x_peer)
    x4.start()
    x4.wait()
    r_mine = pl.ds(pl.multiple_of(half + core * NB, NB), NB)
    r_theirs = pl.ds(pl.multiple_of(half + (1 - core) * NB, NB), NB)
    inv_cols = t_buf[half:, pl.ds(pl.multiple_of((3 - c) * NB, NB), NB)]
    done_s[...] = r_ref[half:, r_mine] + dot_nn(inv_cols, tail_s[...] + tail_r[1])
    x5 = pair_copy(done_s, done_r, 6, core_peer)
    x5.start()
    r_ref[half:, r_mine] = done_s[...]
    send_rows(c * half_rows, half_rows, pl.ds(0, half), ya_send, ya_recv.at[0]).wait_send()
    for l in range(2):
        send_rows(other * half_rows, half_rows, pl.ds(l * NB, NB), yb_send.at[l], yb_recv.at[l, 0]).wait_send()
    x5.wait()
    r_ref[half:, r_theirs] = done_r[...]


def gram_rows(a_loc, diag_shift):
    rows, cols = a_loc.shape
    half = cols // 2
    kk = cols
    qr = half // 4
    dma = pltpu.SemaphoreType.DMA
    vm = lambda *shape: pltpu.VMEM(shape, F32)
    return pl.pallas_call(
        gram_kernel,
        out_shape=(pltpu.VMEM((kk, cols), F32), pltpu.SMEM((1, 1), jnp.int32)),
        in_specs=[pl.BlockSpec(memory_space=pl.ANY), pl.BlockSpec(memory_space=pl.ANY)],
        out_specs=(pl.BlockSpec(memory_space=pltpu.VMEM), pl.BlockSpec(memory_space=pltpu.SMEM)),
        scratch_shapes=[
            vm(*diag_shift.shape), vm(rows, cols), vm(rows, half), vm(half, cols), vm(half, cols), vm(2, half, cols),
            vm(2, 4, 3 * NB // 4 + 8, NB), vm(4, qr, half), vm(3, qr, half), vm(qr, half), vm(4, qr, half),
            vm(2, NB, half), vm(2, NB, half), vm(2, NB, NB), vm(NB, NB), vm(half, NB), vm(half, NB),
            vm(kk, kk), vm(kk, kk), vm(kk, kk), vm(kk, half), vm(8, half), vm(NB, NB), vm(NB, NB),
            dma((4,)), dma, dma((rows // 1024,)), dma((2,)), dma((2, 4)), dma((7,)), dma((7,)), dma, dma, dma((3,)), dma((3,)),
            dma((3,)), dma((3,)), dma, dma, dma((3,)), dma((3,)), dma,
        ],
        compiler_params=pltpu.CompilerParams(collective_id=0, has_side_effects=True, vmem_limit_bytes=48 * 1024 * 1024),
        name='gram_rows',
    )(a_loc, diag_shift)


def solution(mesh):
    n_pcol = mesh.shape['pcol']

    def local_qr(a_loc, diag_shift):
        rows, ok = gram_rows(a_loc, diag_shift)
        return lax.cond(ok[0, 0] != 0, lambda a, s, r: r, lambda a, s, r: householder_rows(a, s, n_pcol), a_loc, diag_shift, rows)

    return jax.shard_map(local_qr, mesh=mesh, in_specs=(P(('batch', 'prow'), 'pcol'), P('batch', None)), out_specs=P('batch', 'pcol'), check_vma=False)
```

```python
import functools

import jax
import jax.numpy as jnp
from jax import lax
from jax.experimental import pallas as pl
from jax.experimental.pallas import tpu as pltpu
from jax.sharding import PartitionSpec as P

PRECISE = lax.Precision.HIGHEST
F32 = jnp.float32
NB = 128
MESH = pl.DeviceIdType.MESH
TRACE_FACTOR = 2.0


def dot_nn(x, y):
    return lax.dot_general(x, y, (((1,), (0,)), ((), ())), precision=PRECISE, preferred_element_type=F32)


def dot_tn(x, y):
    return lax.dot_general(x, y, (((0,), (0,)), ((), ())), precision=PRECISE, preferred_element_type=F32)


def gather_sum(x, axis):
    return jnp.sum(lax.all_gather(x, axis), axis=0)


def factor_panel(panel, glob_rows, col_base):
    blocksize = panel.shape[1]
    lane_ids = jnp.arange(blocksize)

    def col_step(k, loop_state):
        panel, vectors, tau_vec, sign_vec = loop_state
        glob_col = col_base + k
        active = glob_rows >= glob_col
        is_pivot = glob_rows == glob_col
        column = lax.dynamic_slice_in_dim(panel, k, 1, axis=1)[:, 0]
        reduced = gather_sum(jnp.stack([jnp.sum(jnp.where(active, column, 0.0)[:, None] * panel, axis=0),
                                        jnp.sum(jnp.where(is_pivot[:, None], panel, 0.0), axis=0)]), 'prow')
        col_dots = reduced[0]
        pivot_row = reduced[1]
        pivot_val = lax.dynamic_index_in_dim(pivot_row, k, keepdims=False)
        col_norm = jnp.sqrt(lax.dynamic_index_in_dim(col_dots, k, keepdims=False))
        beta_val = jnp.where(pivot_val >= 0, -col_norm, col_norm)
        tau_val = (beta_val - pivot_val) / beta_val
        inv_scale = 1.0 / (pivot_val - beta_val)
        v_col = jnp.where(is_pivot, 1.0, jnp.where(active, column * inv_scale, 0.0))
        v_dots = inv_scale * (col_dots - pivot_val * pivot_row) + pivot_row
        update = jnp.where(lane_ids > k, tau_val * v_dots, 0.0)
        new_col = jnp.where(active, jnp.where(is_pivot, beta_val, 0.0), column)
        panel = panel - v_col[:, None] * update[None, :]
        panel = lax.dynamic_update_slice_in_dim(panel, new_col[:, None], k, axis=1)
        vectors = lax.dynamic_update_slice_in_dim(vectors, v_col[:, None], k, axis=1)
        tau_vec = jnp.where(lane_ids == k, tau_val, tau_vec)
        sign_vec = jnp.where(lane_ids == k, jnp.where(beta_val < 0, -1.0, 1.0), sign_vec)
        return panel, vectors, tau_vec, sign_vec

    init_state = (panel, jnp.zeros_like(panel), jnp.zeros((blocksize,), F32), jnp.zeros((blocksize,), F32))
    return lax.fori_loop(0, blocksize, col_step, init_state)


def build_tfactor(gram_mat, tau_vec):
    blocksize = tau_vec.shape[0]
    lane_ids = jnp.arange(blocksize)

    def t_step(k, t_factor):
        gram_col = jnp.where(lane_ids < k, lax.dynamic_slice_in_dim(gram_mat, k, 1, axis=1)[:, 0], 0.0)
        tau_k = lax.dynamic_index_in_dim(tau_vec, k, keepdims=False)
        column = -tau_k * jnp.sum(t_factor * gram_col[None, :], axis=1)
        column = jnp.where(lane_ids == k, tau_k, column)
        return jnp.where(lane_ids[None, :] == k, column[:, None], t_factor)

    return lax.fori_loop(0, blocksize, t_step, jnp.zeros((blocksize, blocksize), F32))


def householder_rows(a_loc, diag_shift, n_pcol):
    rows_loc, cols_loc = a_loc.shape
    panels, blocksize = diag_shift.shape
    total_k = panels * blocksize
    row_id = lax.axis_index('prow')
    col_id = lax.axis_index('pcol')
    glob_rows = row_id * rows_loc + jnp.arange(rows_loc)
    local_cols = jnp.arange(cols_loc)
    orig_cols = ((local_cols // blocksize) * n_pcol + col_id) * blocksize + local_cols % blocksize
    shift_flat = diag_shift.reshape(total_k)
    col_shift = jnp.where(orig_cols < total_k, shift_flat[jnp.minimum(orig_cols, total_k - 1)], 0.0)
    a_loc = a_loc + jnp.where(glob_rows[:, None] == orig_cols[None, :], col_shift[None, :], 0.0)
    swap = [(0, 1), (1, 0)]

    def owned(x, is_owner):
        return jnp.where(is_owner, x, lax.ppermute(x, 'pcol', swap))

    def panel_step(panel_idx, state):
        a_loc, signs = state
        owner_col = panel_idx % n_pcol
        start_col = (panel_idx // n_pcol) * blocksize
        is_owner = col_id == owner_col
        panel = lax.dynamic_slice_in_dim(a_loc, start_col, blocksize, axis=1)
        factored, vectors, tau_vec, sign_vec = factor_panel(panel, glob_rows, panel_idx * blocksize)
        vectors, scalars = owned(vectors, is_owner), owned(jnp.stack([tau_vec, sign_vec]), is_owner)
        tau_vec, sign_vec = scalars[0], scalars[1]
        signs = lax.dynamic_update_slice_in_dim(signs, sign_vec, panel_idx * blocksize, axis=0)
        keep_cols = orig_cols >= (panel_idx + 1) * blocksize
        proj = jnp.einsum('mi,mn->in', vectors, jnp.concatenate([vectors, a_loc], axis=1), precision=PRECISE, preferred_element_type=F32)
        pieces = cols_loc // blocksize + 1
        sums = lax.map(lambda x: gather_sum(x, 'prow'), jnp.swapaxes(proj.reshape(blocksize, pieces, blocksize), 0, 1))
        t_factor = build_tfactor(sums[0], tau_vec)
        proj_sum = jnp.swapaxes(sums[1:], 0, 1).reshape(blocksize, cols_loc)
        w_mat = jnp.where(keep_cols[None, :], jnp.einsum('ij,in->jn', t_factor, proj_sum, precision=PRECISE, preferred_element_type=F32), 0.0)
        a_loc = a_loc - jnp.dot(vectors, w_mat, precision=PRECISE, preferred_element_type=F32)
        kept = lax.dynamic_slice_in_dim(a_loc, start_col, blocksize, axis=1)
        a_loc = lax.dynamic_update_slice_in_dim(a_loc, jnp.where(is_owner, factored, kept), start_col, axis=1)
        return a_loc, signs

    a_loc, signs = lax.fori_loop(0, panels, panel_step, (a_loc, jnp.zeros((total_k,), F32)))
    step = total_k // 8

    def top_step(i, top):
        piece = lax.all_gather(lax.dynamic_slice_in_dim(a_loc, i * step, step, axis=0), 'prow')[0]
        return lax.dynamic_update_slice_in_dim(top, piece, i * step, axis=0)

    top_rows = lax.fori_loop(0, 8, top_step, jnp.zeros((total_k, cols_loc), F32))
    return top_rows * signs[:, None]


def factor_block(block, u_ref, m_ref):
    sub = lax.broadcasted_iota(jnp.int32, (8, NB), 0)
    lane = lax.broadcasted_iota(jnp.int32, (8, NB), 1)
    eye = (lax.broadcasted_iota(jnp.int32, (NB, NB), 0) == lax.broadcasted_iota(jnp.int32, (NB, NB), 1)).astype(F32)
    wide = lambda row: jnp.broadcast_to(row, (8, NB))

    def group(tiles, g, state):
        s_tiles, m_tiles = state[:tiles], state[tiles:]
        base = pl.multiple_of(g * 8, 8)
        spread = lambda tile, t: jnp.take_along_axis(tile, jnp.full((8, NB), base + t, jnp.int32), axis=1)
        s_top, m_top = s_tiles[0], m_tiles[0]
        cols = [spread(s_top, t) for t in range(8)]
        dinv = jnp.zeros((8, NB), F32)
        for s in range(8):
            inv_p = 1.0 / wide(cols[s][s:s + 1])
            dinv = jnp.where(sub == s, inv_p, dinv)
            mult = jnp.where(sub > s, cols[s] * inv_p, 0.0)
            for t in range(s + 1, 8):
                cols[t] = cols[t] - mult * wide(cols[t][s:s + 1])
            s_top = s_top - mult * wide(s_top[s:s + 1])
            m_top = m_top - mult * wide(m_top[s:s + 1])
        scale = jnp.sqrt(dinv)
        u_ref[pl.ds(base, 8), :] = jnp.where(lane >= sub + base, s_top * scale, 0.0)
        m_ref[pl.ds(base, 8), :] = m_top * scale
        s_sol, m_sol = s_top * dinv, m_top * dinv
        for s in range(7, 0, -1):
            mult = jnp.where(sub < s, cols[s] * dinv, 0.0)
            s_sol = s_sol - mult * wide(s_sol[s:s + 1])
            m_sol = m_sol - mult * wide(m_sol[s:s + 1])
        s_rows = [wide(s_sol[t:t + 1]) for t in range(8)]
        m_rows = [wide(m_sol[t:t + 1]) for t in range(8)]
        s_new, m_new = [], []
        for v in range(1, tiles):
            s_acc, m_acc = s_tiles[v], m_tiles[v]
            for t in range(8):
                col = spread(s_tiles[v], t)
                s_acc = s_acc - col * s_rows[t]
                m_acc = m_acc - col * m_rows[t]
            s_new.append(s_acc)
            m_new.append(m_acc)
        zero = jnp.zeros((8, NB), F32)
        return tuple(s_new + [zero] + m_new + [zero])

    def tiles_of(x):
        return [x[8 * v:8 * v + 8] for v in range(x.shape[0] // 8)]

    n = NB // 8
    state = tuple(tiles_of(block) + tiles_of(eye))
    done = 0
    for tiles, steps in ((n, n // 2), (n // 2, n // 2)):
        state = lax.fori_loop(done, done + steps, functools.partial(group, tiles), state)
        done += steps
        half = len(state) // 2
        state = state[:n - done] + state[half:half + n - done]


def gram_kernel(a_hbm, s_hbm, r_ref, ok_ref, s_ref, own, peer, pack, pack_r, acc1, acc2, acc1_r, hb, cm_buf, cm_recv, cy_recv, cfin,
                xp, xp_r, xg, xg_r, k_first, k_last, tail_r, tail_s, done_s, done_r, z_buf, t_buf, rf_buf, k12, ymax, u_blk, m_blk,
                load_sem, ya_send, ya_recv, yb_send, yb_recv, yp_send, yp_recv, ar_send, ar_recv, gy_send, gy_recv, gq_send, gq_recv,
                rs_send, rs_recv, cy_send, cy_rsem, ag_send, ag_recv, s_sem):
    rows, cols = a_hbm.shape
    half_rows = rows // 2
    half = cols // 2
    kk = 2 * half
    c = lax.axis_index('pcol')
    p = lax.axis_index('prow')
    other = 1 - c
    core = p % 2
    core_peer = p + 1 - 2 * core
    x_peer = (p + 2) % 4
    qr = half // 4
    qb = NB // 4
    ca = 512
    n_a = half_rows // ca
    n_l = rows // ca
    per_load = n_l // 4
    b_cuts = (0, 768, 1920, 3072)
    n_b = len(b_cuts) - 1
    n_g = 4
    wg = NB // n_g
    rq = half_rows // n_g
    last_cuts = (0, 512, 640, 704, 768)
    p_cuts = [(g, 0, rq) for g in range(n_g - 1)] + [(n_g - 1, lo, hi) for lo, hi in zip(last_cuts, last_cuts[1:])]

    def row0(start, size):
        return pl.ds(pl.multiple_of(start, NB), size)

    def to_prow(src, dst, send, recv, q):
        return pltpu.make_async_remote_copy(src, dst, send, recv, device_id={'prow': q}, device_id_type=MESH)

    def to_pcol(src, dst, send, recv):
        return pltpu.make_async_remote_copy(src, dst, send, recv, device_id={'pcol': other}, device_id_type=MESH)

    def load(g):
        rs = row0(g * per_load * ca, per_load * ca)
        return pltpu.make_async_copy(a_hbm.at[rs, :], own.at[rs, :], load_sem.at[g])

    barrier = pltpu.get_barrier_semaphore()
    pl.semaphore_signal(barrier, inc=1, device_id={'pcol': other}, device_id_type=MESH)
    for d in range(1, 4):
        pl.semaphore_signal(barrier, inc=1, device_id={'prow': (p + d) % 4}, device_id_type=MESH)
    s_load = pltpu.make_async_copy(s_hbm, s_ref, s_sem)
    s_load.start()
    for g in range(4):
        load(g).start()
    pl.semaphore_wait(barrier, 4)

    def send_rows(start, size, lanes, send, recv):
        rs = row0(start, size)
        return to_pcol(a_hbm.at[rs, lanes], peer.at[rs, lanes], send, recv)

    def send_a(k):
        return send_rows(c * half_rows + k * ca, ca, pl.ds(0, half), ya_send, ya_recv.at[k])

    def send_b(k):
        lo, hi = b_cuts[k], b_cuts[k + 1]
        return send_rows(other * half_rows + lo, hi - lo, pl.ds(0, NB), yb_send, yb_recv.at[k])

    def send_p(i):
        g, lo, hi = p_cuts[i]
        return to_pcol(pack.at[g, pl.ds(lo, hi - lo), :], pack_r.at[g, pl.ds(lo, hi - lo), :], yp_send, yp_recv.at[i])

    for k in range(4):
        send_a(k).start()

    eye = (lax.broadcasted_iota(jnp.int32, (NB, NB), 0) == lax.broadcasted_iota(jnp.int32, (NB, NB), 1)).astype(F32)

    def add_shift(ref, side, l, cond):
        @pl.when(jnp.logical_and(p == 0, cond))
        def _():
            panel = 2 * l + side
            rs = row0(panel * NB, NB)
            ref[rs, l * NB:(l + 1) * NB] = ref[rs, l * NB:(l + 1) * NB] + eye * s_ref[pl.ds(panel, 1), :]

    acc1[...] = jnp.zeros_like(acc1)
    acc2[...] = jnp.zeros_like(acc2)
    ymax[...] = jnp.zeros_like(ymax)
    s_load.wait()

    @pl.loop(0, n_l)
    def _(j):
        @pl.when(j % per_load == 0)
        def _():
            load(j // per_load).wait()

        for l in range(2):
            add_shift(own, c, l, j == 0)
        rs = pl.ds(pl.multiple_of(j * ca, ca), ca)
        right = own[rs, :]
        ymax[...] = jnp.maximum(ymax[...], jnp.max(jnp.abs(right[:, half:]).reshape(ca // 8, 8, half), axis=0))
        acc1[...] += dot_tn(right[:, :half], right)

    acc1[NB:NB + 8, :NB] = jnp.maximum(ymax[:, :NB], ymax[:, NB:])

    def pair_copy(src, dst, slot, q):
        return to_prow(src, dst, ar_send.at[slot], ar_recv.at[slot], q)

    g1 = pair_copy(acc1, acc1_r.at[0], 0, core_peer)
    g1.start()
    g1.wait()
    acc1[...] += acc1_r[0]
    g2 = pair_copy(acc1, acc1_r.at[1], 1, x_peer)
    g2.start()

    group_of = lax.broadcasted_iota(jnp.int32, (rq // 8, NB), 1) // wg

    @pl.loop(0, 8)
    def _(i):
        step = rq // 8
        parts = [own[pl.ds(pl.multiple_of(other * half_rows + q * rq + i * step, 8), step), NB:half] for q in range(n_g)]
        for g in range(n_g):
            packed = jnp.zeros((step, NB), F32)
            for q in range(n_g):
                turn = wg * ((q - g) % n_g)
                packed = jnp.where(group_of == q, pltpu.roll(parts[q], turn, 1) if turn else parts[q], packed)
            pack[g, pl.ds(pl.multiple_of(i * step, 8), step), :] = packed

    g2.wait()
    acc1[...] += acc1_r[1]
    for q in range(4):
        rs = slice(q * qb, (q + 1) * qb)
        hb[c, q, :qb, :] = acc1[rs, :NB]
        hb[c, q, qb:2 * qb, :] = acc1[rs, NB:half]
        hb[c, q, 2 * qb:3 * qb, :] = acc1[NB + q * qb:NB + (q + 1) * qb, NB:half]
        hb[c, q, 3 * qb:, :] = acc1[NB:NB + 8, :NB]
    gy = to_pcol(hb.at[c, p], hb.at[c, p], gy_send, gy_recv)
    gy.start()
    for k in range(4, n_a):
        send_a(k).start()
    send_b(0).start()

    def gram_block(side, b):
        return jnp.concatenate([hb[side, q, b * qb:(b + 1) * qb, :] for q in range(4)], axis=0)

    def take_a(k):
        send_a(k).wait_recv()
        for l in range(2):
            add_shift(peer, other, l, jnp.logical_and(c == 1, k == 0))
        rs = row0(other * half_rows + k * ca, ca)
        acc2[...] += dot_tn(peer[rs, :], own[rs, :])

    def spread_gram(d, src):
        return to_prow(hb.at[other, src], hb.at[other, src], gq_send.at[d - 1], gq_recv.at[d - 1], (p + d) % 4)

    @pl.loop(0, n_a)
    def _(k):
        take_a(k)

        @pl.when(k == n_a - 3)
        def _():
            gy.wait()
            for d in range(1, 4):
                spread_gram(d, p).start()

        @pl.when(k == n_a - 2)
        def _():
            for d in range(1, 4):
                spread_gram(d, p).wait_send()
                spread_gram(d, (p + 4 - d) % 4).wait_recv()
            factor_block(gram_block(0, 0), u_blk, m_blk)

    @pl.when(c == 0)
    def _():
        ct = acc2[:, :half].T
        for q in range(4):
            cm_buf[q] = ct[q * qr:(q + 1) * qr]

    @pl.when(c == 1)
    def _():
        for q in range(4):
            cm_buf[q] = acc2[q * qr:(q + 1) * qr, :half]

    def scatter(d):
        q = (p + d) % 4
        return to_prow(cm_buf.at[q], cm_recv.at[d - 1], rs_send.at[d - 1], rs_recv.at[d - 1], q)

    for d in range(1, 4):
        scatter(d).start()
    xp[...] = acc2[:NB, half:]
    for g in range(n_g):
        xg[g] = acc2[NB + g * wg:NB + (g + 1) * wg, half:]
    k_first[...] = jnp.zeros_like(k_first)
    k_last[...] = jnp.zeros_like(k_last)
    for d in range(1, 4):
        scatter(d).wait()
    cm_buf[p] = ((cm_buf[p] + cm_recv[0]) + cm_recv[1]) + cm_recv[2]
    cy = to_pcol(cm_buf.at[p], cy_recv, cy_send, cy_rsem)
    cy.start()
    for k in range(1, n_b):
        send_b(k).start()
    for i in range(len(p_cuts)):
        send_p(i).start()
    cy.wait()
    cfin[p] = cm_buf[p] + cy_recv[...]

    def spread(d, src):
        return to_prow(cfin.at[src], cfin.at[src], ag_send.at[d - 1], ag_recv.at[d - 1], (p + d) % 4)

    for d in range(1, 4):
        spread(d, p).start()
    for d in range(1, 4):
        spread(d, p).wait_send()
        spread(d, (p + 4 - d) % 4).wait_recv()

    cross = jnp.concatenate([cfin[q] for q in range(4)], axis=0)
    z_buf[...] = jnp.zeros_like(z_buf)
    diag_max = jnp.zeros((1, NB), F32)
    diag_min = jnp.full((1, NB), jnp.inf, F32)
    diags = []
    for i in range(4):
        ci, li = i % 2, i // 2
        for j in range(i, 4):
            cj, lj = j % 2, j // 2
            if ci == cj:
                block = gram_block(ci, li + lj)
            elif ci == 0:
                block = cross[li * NB:(li + 1) * NB, lj * NB:(lj + 1) * NB]
            else:
                block = cross[lj * NB:(lj + 1) * NB, li * NB:(li + 1) * NB].T
            z_buf[i * NB:(i + 1) * NB, j * NB:(j + 1) * NB] = block
            if i == j:
                d_row = jnp.sum(block * eye, axis=0, keepdims=True)
                diags.append(d_row)
                diag_max = jnp.maximum(diag_max, d_row)
                diag_min = jnp.minimum(diag_min, d_row)

    t_buf[...] = jnp.zeros_like(t_buf)
    rf_buf[...] = jnp.zeros_like(rf_buf)
    for j in range(4):
        lo, hi = j * NB, (j + 1) * NB
        if j > 0:
            factor_block(z_buf[lo:hi, lo:hi], u_blk, m_blk)
        inv_t = m_blk[...]
        rf_buf[lo:hi, lo:hi] = u_blk[...]
        t_buf[lo:hi, lo:hi] = inv_t
        new_row = dot_nn(inv_t, z_buf[lo:hi, :])
        if j > 0:
            t_buf[lo:hi, :lo] = new_row[:, :lo]
        if j < 3:
            rf_buf[lo:hi, hi:] = new_row[:, hi:]
            parts = ([new_row[:, :lo]] if j > 0 else []) + [inv_t, new_row[:, hi:]]
            mult = jnp.concatenate(parts, axis=1)
            z_buf[hi:, lo:hi] = jnp.zeros((kk - hi, NB), F32)
            z_buf[hi:, :] = z_buf[hi:, :] - dot_tn(new_row[:, hi:], mult)

    trace = jnp.zeros((1, NB), F32)
    for i in range(4):
        tc = t_buf[i * NB:, i * NB:(i + 1) * NB]
        trace = trace + jnp.sum(tc * tc, axis=0, keepdims=True) * diags[i]
    total = jnp.sum(trace, axis=1, keepdims=True)
    d_max = jnp.max(diag_max, axis=1, keepdims=True)
    d_min = jnp.min(diag_min, axis=1, keepdims=True)
    y_max = jnp.maximum(hb[0, 0, 3 * qb:, :], hb[1, 0, 3 * qb:, :])
    y_max = jnp.max(jnp.max(y_max, axis=0, keepdims=True), axis=1, keepdims=True)
    good = (total < TRACE_FACTOR * kk) & (d_min > 1e-26) & (d_max < 1e36) & (y_max * jnp.sqrt(d_max) < 1e33)
    ok_ref[0, 0] = jnp.where(good, 1, 0)[0, 0]

    for l in range(2):
        ls = pl.ds(pl.multiple_of((2 * l + c) * NB, NB), NB)
        r_ref[:, l * NB:(l + 1) * NB] = rf_buf[:, ls]

    k12[row0(c * NB, NB), :] = acc1[:NB, half:]
    k12[row0((c + 2) * NB, NB), :] = acc1[NB:, half:]
    k12[row0((3 - c) * NB, NB), :] = jnp.zeros((NB, half), F32)

    for k in range(n_b):
        send_b(k).wait_recv()
        if k == 0:
            add_shift(peer, other, 0, c == 0)
        rs = row0(c * half_rows + b_cuts[k], b_cuts[k + 1] - b_cuts[k])
        xp[...] += dot_tn(peer[rs, :NB], own[rs, half:])
    x1 = pair_copy(xp, xp_r.at[0], 2, core_peer)
    x1.start()
    x1.wait()
    xp[...] = xp[...] + xp_r[0]
    x2 = pair_copy(xp, xp_r.at[1], 3, x_peer)
    x2.start()
    x2.wait()
    k12[row0((1 - c) * NB, NB), :] = xp[...] + xp_r[1]
    r_ref[:, half:] = dot_nn(t_buf[...], k12[...])

    def take_p(g, lo, hi):
        turned = pack_r[g, lo:hi, :].T
        for q in range(n_g):
            rs = pl.ds(pl.multiple_of(c * half_rows + q * rq + lo, 8), hi - lo)
            xg[g] += dot_nn(turned[q * wg:(q + 1) * wg, :], own[rs, half:])

    inv_cols = t_buf[half:, pl.ds(pl.multiple_of((3 - c) * NB, NB), NB)]

    @pl.loop(0, n_g - 1)
    def _(g):
        to_pcol(pack.at[g], pack_r.at[g], yp_send, yp_recv.at[g]).wait_recv()
        take_p(g, 0, rq)
        x3 = pair_copy(xg.at[g], xg_r.at[0, g], 4 + 2 * g, core_peer)
        x3.start()
        x3.wait()
        xg[g] = xg[g] + xg_r[0, g]
        x4 = pair_copy(xg.at[g], xg_r.at[1, g], 5 + 2 * g, x_peer)
        x4.start()
        x4.wait()
        k_first[pl.ds(pl.multiple_of(g * wg, wg), wg), :] = xg[g] + xg_r[1, g]

    r_ref[half:, half:] += dot_nn(inv_cols, k_first[...])
    for i in range(n_g - 1, len(p_cuts)):
        send_p(i).wait_recv()
        take_p(*p_cuts[i])
    g = n_g - 1
    mine = pl.ds(pl.multiple_of(core * NB, NB), NB)
    theirs = pl.ds(pl.multiple_of((1 - core) * NB, NB), NB)
    x5 = pair_copy(xg.at[g, :, theirs], tail_r.at[0], 10, core_peer)
    x5.start()
    x5.wait()
    tail_s[...] = xg[g, :, mine] + tail_r[0]
    x6 = pair_copy(tail_s, tail_r.at[1], 11, x_peer)
    x6.start()
    x6.wait()
    k_last[g * wg:, :] = tail_s[...] + tail_r[1]
    r_mine = pl.ds(pl.multiple_of(half + core * NB, NB), NB)
    r_theirs = pl.ds(pl.multiple_of(half + (1 - core) * NB, NB), NB)
    done_s[...] = r_ref[half:, r_mine] + dot_nn(inv_cols, k_last[...])
    x7 = pair_copy(done_s, done_r, 12, core_peer)
    x7.start()
    r_ref[half:, r_mine] = done_s[...]
    send_rows(c * half_rows, half_rows, pl.ds(0, half), ya_send, ya_recv.at[0]).wait_send()
    send_rows(other * half_rows, half_rows, pl.ds(0, NB), yb_send, yb_recv.at[0]).wait_send()
    to_pcol(pack, pack_r, yp_send, yp_recv.at[0]).wait_send()
    x7.wait()
    r_ref[half:, r_theirs] = done_r[...]


def gram_rows(a_loc, diag_shift):
    rows, cols = a_loc.shape
    half = cols // 2
    kk = cols
    qr = half // 4
    dma = pltpu.SemaphoreType.DMA
    vm = lambda *shape: pltpu.VMEM(shape, F32)
    return pl.pallas_call(
        gram_kernel,
        out_shape=(pltpu.VMEM((kk, cols), F32), pltpu.SMEM((1, 1), jnp.int32)),
        in_specs=[pl.BlockSpec(memory_space=pl.ANY), pl.BlockSpec(memory_space=pl.ANY)],
        out_specs=(pl.BlockSpec(memory_space=pltpu.VMEM), pl.BlockSpec(memory_space=pltpu.SMEM)),
        scratch_shapes=[
            vm(*diag_shift.shape), vm(rows, cols), vm(rows, half), vm(4, rows // 8, NB), vm(4, rows // 8, NB), vm(half, cols), vm(half, cols), vm(2, half, cols),
            vm(2, 4, 3 * NB // 4 + 8, NB), vm(4, qr, half), vm(3, qr, half), vm(qr, half), vm(4, qr, half),
            vm(NB, half), vm(2, NB, half), vm(4, NB // 4, half), vm(2, 3, NB // 4, half), vm(NB, half), vm(NB, NB),
            vm(2, NB // 4, NB), vm(NB // 4, NB), vm(half, NB), vm(half, NB),
            vm(kk, kk), vm(kk, kk), vm(kk, kk), vm(kk, half), vm(8, half), vm(NB, NB), vm(NB, NB),
            dma((4,)), dma, dma((rows // 1024,)), dma, dma((3,)), dma, dma((7,)), dma((13,)), dma((13,)), dma, dma, dma((3,)), dma((3,)),
            dma((3,)), dma((3,)), dma, dma, dma((3,)), dma((3,)), dma,
        ],
        compiler_params=pltpu.CompilerParams(collective_id=0, has_side_effects=True, vmem_limit_bytes=48 * 1024 * 1024),
        name='gram_rows',
    )(a_loc, diag_shift)


def solution(mesh):
    n_pcol = mesh.shape['pcol']

    def local_qr(a_loc, diag_shift):
        rows, ok = gram_rows(a_loc, diag_shift)
        return lax.cond(ok[0, 0] != 0, lambda a, s, r: r, lambda a, s, r: householder_rows(a, s, n_pcol), a_loc, diag_shift, rows)

    return jax.shard_map(local_qr, mesh=mesh, in_specs=(P(('batch', 'prow'), 'pcol'), P('batch', None)), out_specs=P('batch', 'pcol'), check_vma=False)
```

```python
import functools

import jax
import jax.numpy as jnp
from jax import lax
from jax.experimental import pallas as pl
from jax.experimental.pallas import tpu as pltpu
from jax.sharding import PartitionSpec as P

PRECISE = lax.Precision.HIGHEST
F32 = jnp.float32
NB = 128
MESH = pl.DeviceIdType.MESH
TRACE_FACTOR = 2.0


def dot_nn(x, y):
    return lax.dot_general(x, y, (((1,), (0,)), ((), ())), precision=PRECISE, preferred_element_type=F32)


def dot_tn(x, y):
    return lax.dot_general(x, y, (((0,), (0,)), ((), ())), precision=PRECISE, preferred_element_type=F32)


def gather_sum(x, axis):
    return jnp.sum(lax.all_gather(x, axis), axis=0)


def factor_panel(panel, glob_rows, col_base):
    blocksize = panel.shape[1]
    lane_ids = jnp.arange(blocksize)

    def col_step(k, loop_state):
        panel, vectors, tau_vec, sign_vec = loop_state
        glob_col = col_base + k
        active = glob_rows >= glob_col
        is_pivot = glob_rows == glob_col
        column = lax.dynamic_slice_in_dim(panel, k, 1, axis=1)[:, 0]
        reduced = gather_sum(jnp.stack([jnp.sum(jnp.where(active, column, 0.0)[:, None] * panel, axis=0),
                                        jnp.sum(jnp.where(is_pivot[:, None], panel, 0.0), axis=0)]), 'prow')
        col_dots = reduced[0]
        pivot_row = reduced[1]
        pivot_val = lax.dynamic_index_in_dim(pivot_row, k, keepdims=False)
        col_norm = jnp.sqrt(lax.dynamic_index_in_dim(col_dots, k, keepdims=False))
        beta_val = jnp.where(pivot_val >= 0, -col_norm, col_norm)
        tau_val = (beta_val - pivot_val) / beta_val
        inv_scale = 1.0 / (pivot_val - beta_val)
        v_col = jnp.where(is_pivot, 1.0, jnp.where(active, column * inv_scale, 0.0))
        v_dots = inv_scale * (col_dots - pivot_val * pivot_row) + pivot_row
        update = jnp.where(lane_ids > k, tau_val * v_dots, 0.0)
        new_col = jnp.where(active, jnp.where(is_pivot, beta_val, 0.0), column)
        panel = panel - v_col[:, None] * update[None, :]
        panel = lax.dynamic_update_slice_in_dim(panel, new_col[:, None], k, axis=1)
        vectors = lax.dynamic_update_slice_in_dim(vectors, v_col[:, None], k, axis=1)
        tau_vec = jnp.where(lane_ids == k, tau_val, tau_vec)
        sign_vec = jnp.where(lane_ids == k, jnp.where(beta_val < 0, -1.0, 1.0), sign_vec)
        return panel, vectors, tau_vec, sign_vec

    init_state = (panel, jnp.zeros_like(panel), jnp.zeros((blocksize,), F32), jnp.zeros((blocksize,), F32))
    return lax.fori_loop(0, blocksize, col_step, init_state)


def build_tfactor(gram_mat, tau_vec):
    blocksize = tau_vec.shape[0]
    lane_ids = jnp.arange(blocksize)

    def t_step(k, t_factor):
        gram_col = jnp.where(lane_ids < k, lax.dynamic_slice_in_dim(gram_mat, k, 1, axis=1)[:, 0], 0.0)
        tau_k = lax.dynamic_index_in_dim(tau_vec, k, keepdims=False)
        column = -tau_k * jnp.sum(t_factor * gram_col[None, :], axis=1)
        column = jnp.where(lane_ids == k, tau_k, column)
        return jnp.where(lane_ids[None, :] == k, column[:, None], t_factor)

    return lax.fori_loop(0, blocksize, t_step, jnp.zeros((blocksize, blocksize), F32))


def householder_rows(a_loc, diag_shift, n_pcol):
    rows_loc, cols_loc = a_loc.shape
    panels, blocksize = diag_shift.shape
    total_k = panels * blocksize
    row_id = lax.axis_index('prow')
    col_id = lax.axis_index('pcol')
    glob_rows = row_id * rows_loc + jnp.arange(rows_loc)
    local_cols = jnp.arange(cols_loc)
    orig_cols = ((local_cols // blocksize) * n_pcol + col_id) * blocksize + local_cols % blocksize
    shift_flat = diag_shift.reshape(total_k)
    col_shift = jnp.where(orig_cols < total_k, shift_flat[jnp.minimum(orig_cols, total_k - 1)], 0.0)
    a_loc = a_loc + jnp.where(glob_rows[:, None] == orig_cols[None, :], col_shift[None, :], 0.0)
    swap = [(0, 1), (1, 0)]

    def owned(x, is_owner):
        return jnp.where(is_owner, x, lax.ppermute(x, 'pcol', swap))

    def panel_step(panel_idx, state):
        a_loc, signs = state
        owner_col = panel_idx % n_pcol
        start_col = (panel_idx // n_pcol) * blocksize
        is_owner = col_id == owner_col
        panel = lax.dynamic_slice_in_dim(a_loc, start_col, blocksize, axis=1)
        factored, vectors, tau_vec, sign_vec = factor_panel(panel, glob_rows, panel_idx * blocksize)
        vectors, scalars = owned(vectors, is_owner), owned(jnp.stack([tau_vec, sign_vec]), is_owner)
        tau_vec, sign_vec = scalars[0], scalars[1]
        signs = lax.dynamic_update_slice_in_dim(signs, sign_vec, panel_idx * blocksize, axis=0)
        keep_cols = orig_cols >= (panel_idx + 1) * blocksize
        proj = jnp.einsum('mi,mn->in', vectors, jnp.concatenate([vectors, a_loc], axis=1), precision=PRECISE, preferred_element_type=F32)
        pieces = cols_loc // blocksize + 1
        sums = lax.map(lambda x: gather_sum(x, 'prow'), jnp.swapaxes(proj.reshape(blocksize, pieces, blocksize), 0, 1))
        t_factor = build_tfactor(sums[0], tau_vec)
        proj_sum = jnp.swapaxes(sums[1:], 0, 1).reshape(blocksize, cols_loc)
        w_mat = jnp.where(keep_cols[None, :], jnp.einsum('ij,in->jn', t_factor, proj_sum, precision=PRECISE, preferred_element_type=F32), 0.0)
        a_loc = a_loc - jnp.dot(vectors, w_mat, precision=PRECISE, preferred_element_type=F32)
        kept = lax.dynamic_slice_in_dim(a_loc, start_col, blocksize, axis=1)
        a_loc = lax.dynamic_update_slice_in_dim(a_loc, jnp.where(is_owner, factored, kept), start_col, axis=1)
        return a_loc, signs

    a_loc, signs = lax.fori_loop(0, panels, panel_step, (a_loc, jnp.zeros((total_k,), F32)))
    step = total_k // 8

    def top_step(i, top):
        piece = lax.all_gather(lax.dynamic_slice_in_dim(a_loc, i * step, step, axis=0), 'prow')[0]
        return lax.dynamic_update_slice_in_dim(top, piece, i * step, axis=0)

    top_rows = lax.fori_loop(0, 8, top_step, jnp.zeros((total_k, cols_loc), F32))
    return top_rows * signs[:, None]


def factor_block(block, u_ref, m_ref):
    sub = lax.broadcasted_iota(jnp.int32, (8, NB), 0)
    lane = lax.broadcasted_iota(jnp.int32, (8, NB), 1)
    eye = (lax.broadcasted_iota(jnp.int32, (NB, NB), 0) == lax.broadcasted_iota(jnp.int32, (NB, NB), 1)).astype(F32)
    wide = lambda row: jnp.broadcast_to(row, (8, NB))

    def group(tiles, g, state):
        s_tiles, m_tiles = state[:tiles], state[tiles:]
        base = pl.multiple_of(g * 8, 8)
        spread = lambda tile, t: jnp.take_along_axis(tile, jnp.full((8, NB), base + t, jnp.int32), axis=1)
        s_top, m_top = s_tiles[0], m_tiles[0]
        cols = [spread(s_top, t) for t in range(8)]
        dinv = jnp.zeros((8, NB), F32)
        for s in range(8):
            inv_p = 1.0 / wide(cols[s][s:s + 1])
            dinv = jnp.where(sub == s, inv_p, dinv)
            mult = jnp.where(sub > s, cols[s] * inv_p, 0.0)
            for t in range(s + 1, 8):
                cols[t] = cols[t] - mult * wide(cols[t][s:s + 1])
            s_top = s_top - mult * wide(s_top[s:s + 1])
            m_top = m_top - mult * wide(m_top[s:s + 1])
        scale = jnp.sqrt(dinv)
        u_ref[pl.ds(base, 8), :] = jnp.where(lane >= sub + base, s_top * scale, 0.0)
        m_ref[pl.ds(base, 8), :] = m_top * scale
        s_sol, m_sol = s_top * dinv, m_top * dinv
        for s in range(7, 0, -1):
            mult = jnp.where(sub < s, cols[s] * dinv, 0.0)
            s_sol = s_sol - mult * wide(s_sol[s:s + 1])
            m_sol = m_sol - mult * wide(m_sol[s:s + 1])
        s_rows = [wide(s_sol[t:t + 1]) for t in range(8)]
        m_rows = [wide(m_sol[t:t + 1]) for t in range(8)]
        s_new, m_new = [], []
        for v in range(1, tiles):
            s_acc, m_acc = s_tiles[v], m_tiles[v]
            for t in range(8):
                col = spread(s_tiles[v], t)
                s_acc = s_acc - col * s_rows[t]
                m_acc = m_acc - col * m_rows[t]
            s_new.append(s_acc)
            m_new.append(m_acc)
        zero = jnp.zeros((8, NB), F32)
        return tuple(s_new + [zero] + m_new + [zero])

    def tiles_of(x):
        return [x[8 * v:8 * v + 8] for v in range(x.shape[0] // 8)]

    n = NB // 8
    state = tuple(tiles_of(block) + tiles_of(eye))
    done = 0
    for tiles, steps in ((n, n // 2), (n // 2, n // 2)):
        state = lax.fori_loop(done, done + steps, functools.partial(group, tiles), state)
        done += steps
        half = len(state) // 2
        state = state[:n - done] + state[half:half + n - done]


def gram_kernel(a_hbm, s_hbm, r_ref, ok_ref, s_ref, own, peer, pack, pack_r, fine, fine_r, acc1, acc2, acc1_r, hb, cm_buf, cm_recv, cy_recv, cfin,
                xp, xp_r, xc, xt, z_buf, t_buf, rf_buf, k12, ymax, u_blk, m_blk,
                load_sem, ya_send, ya_recv, yb_send, yb_recv, yp_send, yp_recv, yf_send, yf_recv, fs_send, fs_recv, ar_send, ar_recv, gy_send, gy_recv, gq_send, gq_recv,
                rs_send, rs_recv, cy_send, cy_rsem, ag_send, ag_recv, s_sem):
    rows, cols = a_hbm.shape
    half_rows = rows // 2
    half = cols // 2
    kk = 2 * half
    c = lax.axis_index('pcol')
    p = lax.axis_index('prow')
    other = 1 - c
    core = p % 2
    core_peer = p + 1 - 2 * core
    x_peer = (p + 2) % 4
    qr = half // 4
    qb = NB // 4
    ca = 512
    n_a = half_rows // ca
    n_l = rows // ca
    per_load = n_l // 4
    b_cuts = (0, 768, 1920, 3072)
    n_b = len(b_cuts) - 1
    n_g = 4
    wg = NB // n_g
    rq = half_rows // n_g
    n_f = 2 * n_g
    wf = NB // n_f
    rf = half_rows // n_f
    f_cuts = [(0, 0, rf)] + [(1, lo, hi) for lo, hi in ((0, 256), (256, 352), (352, rf))]

    def row0(start, size):
        return pl.ds(pl.multiple_of(start, NB), size)

    def to_prow(src, dst, send, recv, q):
        return pltpu.make_async_remote_copy(src, dst, send, recv, device_id={'prow': q}, device_id_type=MESH)

    def to_pcol(src, dst, send, recv):
        return pltpu.make_async_remote_copy(src, dst, send, recv, device_id={'pcol': other}, device_id_type=MESH)

    def load(g):
        rs = row0(g * per_load * ca, per_load * ca)
        return pltpu.make_async_copy(a_hbm.at[rs, :], own.at[rs, :], load_sem.at[g])

    barrier = pltpu.get_barrier_semaphore()
    pl.semaphore_signal(barrier, inc=1, device_id={'pcol': other}, device_id_type=MESH)
    for d in range(1, 4):
        pl.semaphore_signal(barrier, inc=1, device_id={'prow': (p + d) % 4}, device_id_type=MESH)
    s_load = pltpu.make_async_copy(s_hbm, s_ref, s_sem)
    s_load.start()
    for g in range(4):
        load(g).start()
    pl.semaphore_wait(barrier, 4)

    def send_rows(start, size, lanes, send, recv):
        rs = row0(start, size)
        return to_pcol(a_hbm.at[rs, lanes], peer.at[rs, lanes], send, recv)

    def send_a(k):
        return send_rows(c * half_rows + k * ca, ca, pl.ds(0, half), ya_send, ya_recv.at[k])

    def send_b(k):
        lo, hi = b_cuts[k], b_cuts[k + 1]
        return send_rows(other * half_rows + lo, hi - lo, pl.ds(0, NB), yb_send, yb_recv.at[k])

    def send_p(g):
        return to_pcol(pack.at[g], pack_r.at[g], yp_send, yp_recv.at[g])

    def send_f(i):
        g, lo, hi = f_cuts[i]
        return to_pcol(fine.at[g, pl.ds(lo, hi - lo), :], fine_r.at[g, pl.ds(lo, hi - lo), :], yf_send, yf_recv.at[i])

    for k in range(4):
        send_a(k).start()

    eye = (lax.broadcasted_iota(jnp.int32, (NB, NB), 0) == lax.broadcasted_iota(jnp.int32, (NB, NB), 1)).astype(F32)

    def add_shift(ref, side, l, cond):
        @pl.when(jnp.logical_and(p == 0, cond))
        def _():
            panel = 2 * l + side
            rs = row0(panel * NB, NB)
            ref[rs, l * NB:(l + 1) * NB] = ref[rs, l * NB:(l + 1) * NB] + eye * s_ref[pl.ds(panel, 1), :]

    acc1[...] = jnp.zeros_like(acc1)
    acc2[...] = jnp.zeros_like(acc2)
    ymax[...] = jnp.zeros_like(ymax)
    s_load.wait()

    @pl.loop(0, n_l)
    def _(j):
        @pl.when(j % per_load == 0)
        def _():
            load(j // per_load).wait()

        for l in range(2):
            add_shift(own, c, l, j == 0)
        rs = pl.ds(pl.multiple_of(j * ca, ca), ca)
        right = own[rs, :]
        ymax[...] = jnp.maximum(ymax[...], jnp.max(jnp.abs(right[:, half:]).reshape(ca // 8, 8, half), axis=0))
        acc1[...] += dot_tn(right[:, :half], right)

    acc1[NB:NB + 8, :NB] = jnp.maximum(ymax[:, :NB], ymax[:, NB:])

    def pair_copy(src, dst, slot, q):
        return to_prow(src, dst, ar_send.at[slot], ar_recv.at[slot], q)

    g1 = pair_copy(acc1, acc1_r.at[0], 0, core_peer)
    g1.start()
    g1.wait()
    acc1[...] += acc1_r[0]
    g2 = pair_copy(acc1, acc1_r.at[1], 1, x_peer)
    g2.start()

    def pack_groups(dst, count, first):
        width = NB // count
        depth = half_rows // count
        step = depth // 8
        group_of = lax.broadcasted_iota(jnp.int32, (step, NB), 1) // width

        @pl.loop(0, 8)
        def _(i):
            packed = [jnp.zeros((step, NB), F32) for _ in range(dst.shape[0])]
            for q in range(count):
                part = own[pl.ds(pl.multiple_of(other * half_rows + q * depth + i * step, 8), step), NB:half]
                for g in range(dst.shape[0]):
                    turn = width * ((q - g - first) % count)
                    packed[g] = jnp.where(group_of == q, pltpu.roll(part, turn, 1) if turn else part, packed[g])
            for g in range(dst.shape[0]):
                dst[g, pl.ds(pl.multiple_of(i * step, 8), step), :] = packed[g]

    pack_groups(pack, n_g, 0)
    pack_groups(fine, n_f, n_f - 2)
    g2.wait()
    acc1[...] += acc1_r[1]
    for q in range(4):
        rs = slice(q * qb, (q + 1) * qb)
        hb[c, q, :qb, :] = acc1[rs, :NB]
        hb[c, q, qb:2 * qb, :] = acc1[rs, NB:half]
        hb[c, q, 2 * qb:3 * qb, :] = acc1[NB + q * qb:NB + (q + 1) * qb, NB:half]
        hb[c, q, 3 * qb:, :] = acc1[NB:NB + 8, :NB]
    gy = to_pcol(hb.at[c, p], hb.at[c, p], gy_send, gy_recv)
    gy.start()
    for k in range(4, n_a):
        send_a(k).start()
    send_b(0).start()

    def gram_block(side, b):
        return jnp.concatenate([hb[side, q, b * qb:(b + 1) * qb, :] for q in range(4)], axis=0)

    def take_a(k):
        send_a(k).wait_recv()
        for l in range(2):
            add_shift(peer, other, l, jnp.logical_and(c == 1, k == 0))
        rs = row0(other * half_rows + k * ca, ca)
        acc2[...] += dot_tn(peer[rs, :], own[rs, :])

    def spread_gram(d, src):
        return to_prow(hb.at[other, src], hb.at[other, src], gq_send.at[d - 1], gq_recv.at[d - 1], (p + d) % 4)

    @pl.loop(0, n_a)
    def _(k):
        take_a(k)

        @pl.when(k == n_a - 3)
        def _():
            gy.wait()
            for d in range(1, 4):
                spread_gram(d, p).start()

        @pl.when(k == n_a - 2)
        def _():
            for d in range(1, 4):
                spread_gram(d, p).wait_send()
                spread_gram(d, (p + 4 - d) % 4).wait_recv()
            factor_block(gram_block(0, 0), u_blk, m_blk)

    @pl.when(c == 0)
    def _():
        ct = acc2[:, :half].T
        for q in range(4):
            cm_buf[q] = ct[q * qr:(q + 1) * qr]

    @pl.when(c == 1)
    def _():
        for q in range(4):
            cm_buf[q] = acc2[q * qr:(q + 1) * qr, :half]

    def scatter(d):
        q = (p + d) % 4
        return to_prow(cm_buf.at[q], cm_recv.at[d - 1], rs_send.at[d - 1], rs_recv.at[d - 1], q)

    for d in range(1, 4):
        scatter(d).start()
    xp[...] = acc2[:NB, half:]
    xc[...] = acc2[NB:, half:]
    for d in range(1, 4):
        scatter(d).wait()
    cm_buf[p] = ((cm_buf[p] + cm_recv[0]) + cm_recv[1]) + cm_recv[2]
    cy = to_pcol(cm_buf.at[p], cy_recv, cy_send, cy_rsem)
    cy.start()
    for k in range(1, n_b):
        send_b(k).start()
    for g in range(n_g - 1):
        send_p(g).start()
    for i in range(len(f_cuts)):
        send_f(i).start()
    cy.wait()
    cfin[p] = cm_buf[p] + cy_recv[...]

    def spread(d, src):
        return to_prow(cfin.at[src], cfin.at[src], ag_send.at[d - 1], ag_recv.at[d - 1], (p + d) % 4)

    for d in range(1, 4):
        spread(d, p).start()
    for d in range(1, 4):
        spread(d, p).wait_send()
        spread(d, (p + 4 - d) % 4).wait_recv()

    cross = jnp.concatenate([cfin[q] for q in range(4)], axis=0)
    z_buf[...] = jnp.zeros_like(z_buf)
    diag_max = jnp.zeros((1, NB), F32)
    diag_min = jnp.full((1, NB), jnp.inf, F32)
    diags = []
    for i in range(4):
        ci, li = i % 2, i // 2
        for j in range(i, 4):
            cj, lj = j % 2, j // 2
            if ci == cj:
                block = gram_block(ci, li + lj)
            elif ci == 0:
                block = cross[li * NB:(li + 1) * NB, lj * NB:(lj + 1) * NB]
            else:
                block = cross[lj * NB:(lj + 1) * NB, li * NB:(li + 1) * NB].T
            z_buf[i * NB:(i + 1) * NB, j * NB:(j + 1) * NB] = block
            if i == j:
                d_row = jnp.sum(block * eye, axis=0, keepdims=True)
                diags.append(d_row)
                diag_max = jnp.maximum(diag_max, d_row)
                diag_min = jnp.minimum(diag_min, d_row)

    t_buf[...] = jnp.zeros_like(t_buf)
    rf_buf[...] = jnp.zeros_like(rf_buf)
    for j in range(4):
        lo, hi = j * NB, (j + 1) * NB
        if j > 0:
            factor_block(z_buf[lo:hi, lo:hi], u_blk, m_blk)
        inv_t = m_blk[...]
        rf_buf[lo:hi, lo:hi] = u_blk[...]
        t_buf[lo:hi, lo:hi] = inv_t
        new_row = dot_nn(inv_t, z_buf[lo:hi, :])
        if j > 0:
            t_buf[lo:hi, :lo] = new_row[:, :lo]
        if j < 3:
            rf_buf[lo:hi, hi:] = new_row[:, hi:]
            parts = ([new_row[:, :lo]] if j > 0 else []) + [inv_t, new_row[:, hi:]]
            mult = jnp.concatenate(parts, axis=1)
            z_buf[hi:, lo:hi] = jnp.zeros((kk - hi, NB), F32)
            z_buf[hi:, :] = z_buf[hi:, :] - dot_tn(new_row[:, hi:], mult)

    trace = jnp.zeros((1, NB), F32)
    for i in range(4):
        tc = t_buf[i * NB:, i * NB:(i + 1) * NB]
        trace = trace + jnp.sum(tc * tc, axis=0, keepdims=True) * diags[i]
    total = jnp.sum(trace, axis=1, keepdims=True)
    d_max = jnp.max(diag_max, axis=1, keepdims=True)
    d_min = jnp.min(diag_min, axis=1, keepdims=True)
    y_max = jnp.maximum(hb[0, 0, 3 * qb:, :], hb[1, 0, 3 * qb:, :])
    y_max = jnp.max(jnp.max(y_max, axis=0, keepdims=True), axis=1, keepdims=True)
    good = (total < TRACE_FACTOR * kk) & (d_min > 1e-26) & (d_max < 1e36) & (y_max * jnp.sqrt(d_max) < 1e33)
    ok_ref[0, 0] = jnp.where(good, 1, 0)[0, 0]

    for l in range(2):
        ls = pl.ds(pl.multiple_of((2 * l + c) * NB, NB), NB)
        r_ref[:, l * NB:(l + 1) * NB] = rf_buf[:, ls]

    k12[row0(c * NB, NB), :] = acc1[:NB, half:]
    k12[row0((c + 2) * NB, NB), :] = acc1[NB:, half:]
    k12[row0((3 - c) * NB, NB), :] = jnp.zeros((NB, half), F32)

    for k in range(n_b):
        send_b(k).wait_recv()
        if k == 0:
            add_shift(peer, other, 0, c == 0)
        rs = row0(c * half_rows + b_cuts[k], b_cuts[k + 1] - b_cuts[k])
        xp[...] += dot_tn(peer[rs, :NB], own[rs, half:])
    x1 = pair_copy(xp, xp_r.at[0], 2, core_peer)
    x1.start()
    x1.wait()
    xp[...] = xp[...] + xp_r[0]
    x2 = pair_copy(xp, xp_r.at[1], 3, x_peer)
    x2.start()
    x2.wait()
    k12[row0((1 - c) * NB, NB), :] = xp[...] + xp_r[1]
    r_ref[:, half:] = dot_nn(t_buf[...], k12[...])

    def take_packed(block, base, depth, start, count, width):
        rs = pl.ds(pl.multiple_of(start, 8), width)
        turned = block.T
        total = xc[rs, :]
        for q in range(count):
            ys = pl.ds(pl.multiple_of(c * half_rows + q * depth + base, 8), block.shape[0])
            total = total + dot_nn(turned[q * width:(q + 1) * width, :], own[ys, half:])
        xc[rs, :] = total

    def share(d, start, size, last):
        rs = pl.ds(pl.multiple_of(start, 8), size)
        return to_prow(xc.at[rs, :], xt.at[p, rs, :], fs_send.at[d - 1], fs_recv.at[last, d - 1], (p + d) % 4)

    @pl.loop(0, n_g - 1)
    def _(g):
        send_p(g).wait_recv()
        take_packed(pack_r[g], 0, rq, g * wg, n_g, wg)
        for d in range(1, 4):
            share(d, g * wg, wg, 0).start()

    inv_cols = t_buf[half:, pl.ds(pl.multiple_of((3 - c) * NB, NB), NB)]
    for i in range(len(f_cuts)):
        g, lo, hi = f_cuts[i]
        start = NB - 2 * wf + g * wf
        send_f(i).wait_recv()
        take_packed(fine_r[g, lo:hi, :], lo, rf, start, n_f, wf)
        if hi == rf:
            for d in range(1, 4):
                share(d, start, wf, g).start()
    xt[p] = xc[...]
    send_rows(c * half_rows, half_rows, pl.ds(0, half), ya_send, ya_recv.at[0]).wait_send()
    send_rows(other * half_rows, half_rows, pl.ds(0, NB), yb_send, yb_recv.at[0]).wait_send()
    to_pcol(pack, pack_r, yp_send, yp_recv.at[0]).wait_send()
    to_pcol(fine, fine_r, yf_send, yf_recv.at[0]).wait_send()
    for d in range(1, 4):
        share(d, 0, NB, 0).wait_send()
        share(d, 0, NB - wf, 0).wait_recv()
    for d in range(1, 4):
        share(d, NB - wf, wf, 1).wait_recv()
    r_ref[half:, half:] += dot_nn(inv_cols, (xt[0] + xt[1]) + (xt[2] + xt[3]))


def gram_rows(a_loc, diag_shift):
    rows, cols = a_loc.shape
    half = cols // 2
    kk = cols
    qr = half // 4
    dma = pltpu.SemaphoreType.DMA
    vm = lambda *shape: pltpu.VMEM(shape, F32)
    return pl.pallas_call(
        gram_kernel,
        out_shape=(pltpu.VMEM((kk, cols), F32), pltpu.SMEM((1, 1), jnp.int32)),
        in_specs=[pl.BlockSpec(memory_space=pl.ANY), pl.BlockSpec(memory_space=pl.ANY)],
        out_specs=(pl.BlockSpec(memory_space=pltpu.VMEM), pl.BlockSpec(memory_space=pltpu.SMEM)),
        scratch_shapes=[
            vm(*diag_shift.shape), vm(rows, cols), vm(rows, half), vm(3, rows // 8, NB), vm(3, rows // 8, NB), vm(2, rows // 16, NB), vm(2, rows // 16, NB), vm(half, cols), vm(half, cols), vm(2, half, cols),
            vm(2, 4, 3 * NB // 4 + 8, NB), vm(4, qr, half), vm(3, qr, half), vm(qr, half), vm(4, qr, half),
            vm(NB, half), vm(2, NB, half), vm(NB, half), vm(4, NB, half),
            vm(kk, kk), vm(kk, kk), vm(kk, kk), vm(kk, half), vm(8, half), vm(NB, NB), vm(NB, NB),
            dma((4,)), dma, dma((rows // 1024,)), dma, dma((3,)), dma, dma((3,)), dma, dma((4,)), dma((3,)), dma((2, 3)), dma((4,)), dma((4,)), dma, dma, dma((3,)), dma((3,)),
            dma((3,)), dma((3,)), dma, dma, dma((3,)), dma((3,)), dma,
        ],
        compiler_params=pltpu.CompilerParams(collective_id=0, has_side_effects=True, vmem_limit_bytes=48 * 1024 * 1024),
        name='gram_rows',
    )(a_loc, diag_shift)


def solution(mesh):
    n_pcol = mesh.shape['pcol']

    def local_qr(a_loc, diag_shift):
        rows, ok = gram_rows(a_loc, diag_shift)
        return lax.cond(ok[0, 0] != 0, lambda a, s, r: r, lambda a, s, r: householder_rows(a, s, n_pcol), a_loc, diag_shift, rows)

    return jax.shard_map(local_qr, mesh=mesh, in_specs=(P(('batch', 'prow'), 'pcol'), P('batch', None)), out_specs=P('batch', 'pcol'), check_vma=False)
```

```python
import functools

import jax
import jax.numpy as jnp
from jax import lax
from jax.experimental import pallas as pl
from jax.experimental.pallas import tpu as pltpu
from jax.sharding import PartitionSpec as P

PRECISE = lax.Precision.HIGHEST
F32 = jnp.float32
NB = 128
MESH = pl.DeviceIdType.MESH
TRACE_FACTOR = 2.0


def dot_nn(x, y):
    return lax.dot_general(x, y, (((1,), (0,)), ((), ())), precision=PRECISE, preferred_element_type=F32)


def dot_tn(x, y):
    return lax.dot_general(x, y, (((0,), (0,)), ((), ())), precision=PRECISE, preferred_element_type=F32)


def gather_sum(x, axis):
    return jnp.sum(lax.all_gather(x, axis), axis=0)


def factor_panel(panel, glob_rows, col_base):
    blocksize = panel.shape[1]
    lane_ids = jnp.arange(blocksize)

    def col_step(k, loop_state):
        panel, vectors, tau_vec, sign_vec = loop_state
        glob_col = col_base + k
        active = glob_rows >= glob_col
        is_pivot = glob_rows == glob_col
        column = lax.dynamic_slice_in_dim(panel, k, 1, axis=1)[:, 0]
        reduced = gather_sum(jnp.stack([jnp.sum(jnp.where(active, column, 0.0)[:, None] * panel, axis=0),
                                        jnp.sum(jnp.where(is_pivot[:, None], panel, 0.0), axis=0)]), 'prow')
        col_dots = reduced[0]
        pivot_row = reduced[1]
        pivot_val = lax.dynamic_index_in_dim(pivot_row, k, keepdims=False)
        col_norm = jnp.sqrt(lax.dynamic_index_in_dim(col_dots, k, keepdims=False))
        beta_val = jnp.where(pivot_val >= 0, -col_norm, col_norm)
        tau_val = (beta_val - pivot_val) / beta_val
        inv_scale = 1.0 / (pivot_val - beta_val)
        v_col = jnp.where(is_pivot, 1.0, jnp.where(active, column * inv_scale, 0.0))
        v_dots = inv_scale * (col_dots - pivot_val * pivot_row) + pivot_row
        update = jnp.where(lane_ids > k, tau_val * v_dots, 0.0)
        new_col = jnp.where(active, jnp.where(is_pivot, beta_val, 0.0), column)
        panel = panel - v_col[:, None] * update[None, :]
        panel = lax.dynamic_update_slice_in_dim(panel, new_col[:, None], k, axis=1)
        vectors = lax.dynamic_update_slice_in_dim(vectors, v_col[:, None], k, axis=1)
        tau_vec = jnp.where(lane_ids == k, tau_val, tau_vec)
        sign_vec = jnp.where(lane_ids == k, jnp.where(beta_val < 0, -1.0, 1.0), sign_vec)
        return panel, vectors, tau_vec, sign_vec

    init_state = (panel, jnp.zeros_like(panel), jnp.zeros((blocksize,), F32), jnp.zeros((blocksize,), F32))
    return lax.fori_loop(0, blocksize, col_step, init_state)


def build_tfactor(gram_mat, tau_vec):
    blocksize = tau_vec.shape[0]
    lane_ids = jnp.arange(blocksize)

    def t_step(k, t_factor):
        gram_col = jnp.where(lane_ids < k, lax.dynamic_slice_in_dim(gram_mat, k, 1, axis=1)[:, 0], 0.0)
        tau_k = lax.dynamic_index_in_dim(tau_vec, k, keepdims=False)
        column = -tau_k * jnp.sum(t_factor * gram_col[None, :], axis=1)
        column = jnp.where(lane_ids == k, tau_k, column)
        return jnp.where(lane_ids[None, :] == k, column[:, None], t_factor)

    return lax.fori_loop(0, blocksize, t_step, jnp.zeros((blocksize, blocksize), F32))


def householder_rows(a_loc, diag_shift, n_pcol):
    rows_loc, cols_loc = a_loc.shape
    panels, blocksize = diag_shift.shape
    total_k = panels * blocksize
    row_id = lax.axis_index('prow')
    col_id = lax.axis_index('pcol')
    glob_rows = row_id * rows_loc + jnp.arange(rows_loc)
    local_cols = jnp.arange(cols_loc)
    orig_cols = ((local_cols // blocksize) * n_pcol + col_id) * blocksize + local_cols % blocksize
    shift_flat = diag_shift.reshape(total_k)
    col_shift = jnp.where(orig_cols < total_k, shift_flat[jnp.minimum(orig_cols, total_k - 1)], 0.0)
    a_loc = a_loc + jnp.where(glob_rows[:, None] == orig_cols[None, :], col_shift[None, :], 0.0)
    swap = [(0, 1), (1, 0)]

    def owned(x, is_owner):
        return jnp.where(is_owner, x, lax.ppermute(x, 'pcol', swap))

    def panel_step(panel_idx, state):
        a_loc, signs = state
        owner_col = panel_idx % n_pcol
        start_col = (panel_idx // n_pcol) * blocksize
        is_owner = col_id == owner_col
        panel = lax.dynamic_slice_in_dim(a_loc, start_col, blocksize, axis=1)
        factored, vectors, tau_vec, sign_vec = factor_panel(panel, glob_rows, panel_idx * blocksize)
        vectors, scalars = owned(vectors, is_owner), owned(jnp.stack([tau_vec, sign_vec]), is_owner)
        tau_vec, sign_vec = scalars[0], scalars[1]
        signs = lax.dynamic_update_slice_in_dim(signs, sign_vec, panel_idx * blocksize, axis=0)
        keep_cols = orig_cols >= (panel_idx + 1) * blocksize
        proj = jnp.einsum('mi,mn->in', vectors, jnp.concatenate([vectors, a_loc], axis=1), precision=PRECISE, preferred_element_type=F32)
        pieces = cols_loc // blocksize + 1
        sums = lax.map(lambda x: gather_sum(x, 'prow'), jnp.swapaxes(proj.reshape(blocksize, pieces, blocksize), 0, 1))
        t_factor = build_tfactor(sums[0], tau_vec)
        proj_sum = jnp.swapaxes(sums[1:], 0, 1).reshape(blocksize, cols_loc)
        w_mat = jnp.where(keep_cols[None, :], jnp.einsum('ij,in->jn', t_factor, proj_sum, precision=PRECISE, preferred_element_type=F32), 0.0)
        a_loc = a_loc - jnp.dot(vectors, w_mat, precision=PRECISE, preferred_element_type=F32)
        kept = lax.dynamic_slice_in_dim(a_loc, start_col, blocksize, axis=1)
        a_loc = lax.dynamic_update_slice_in_dim(a_loc, jnp.where(is_owner, factored, kept), start_col, axis=1)
        return a_loc, signs

    a_loc, signs = lax.fori_loop(0, panels, panel_step, (a_loc, jnp.zeros((total_k,), F32)))
    step = total_k // 8

    def top_step(i, top):
        piece = lax.all_gather(lax.dynamic_slice_in_dim(a_loc, i * step, step, axis=0), 'prow')[0]
        return lax.dynamic_update_slice_in_dim(top, piece, i * step, axis=0)

    top_rows = lax.fori_loop(0, 8, top_step, jnp.zeros((total_k, cols_loc), F32))
    return top_rows * signs[:, None]


def factor_block(block, u_ref, m_ref):
    sub = lax.broadcasted_iota(jnp.int32, (8, NB), 0)
    lane = lax.broadcasted_iota(jnp.int32, (8, NB), 1)
    eye = (lax.broadcasted_iota(jnp.int32, (NB, NB), 0) == lax.broadcasted_iota(jnp.int32, (NB, NB), 1)).astype(F32)
    wide = lambda row: jnp.broadcast_to(row, (8, NB))

    def group(tiles, g, state):
        s_tiles, m_tiles = state[:tiles], state[tiles:]
        base = pl.multiple_of(g * 8, 8)
        spread = lambda tile, t: jnp.take_along_axis(tile, jnp.full((8, NB), base + t, jnp.int32), axis=1)
        s_top, m_top = s_tiles[0], m_tiles[0]
        cols = [spread(s_top, t) for t in range(8)]
        dinv = jnp.zeros((8, NB), F32)
        for s in range(8):
            inv_p = 1.0 / wide(cols[s][s:s + 1])
            dinv = jnp.where(sub == s, inv_p, dinv)
            mult = jnp.where(sub > s, cols[s] * inv_p, 0.0)
            for t in range(s + 1, 8):
                cols[t] = cols[t] - mult * wide(cols[t][s:s + 1])
            s_top = s_top - mult * wide(s_top[s:s + 1])
            m_top = m_top - mult * wide(m_top[s:s + 1])
        scale = jnp.sqrt(dinv)
        u_ref[pl.ds(base, 8), :] = jnp.where(lane >= sub + base, s_top * scale, 0.0)
        m_ref[pl.ds(base, 8), :] = m_top * scale
        s_sol, m_sol = s_top * dinv, m_top * dinv
        for s in range(7, 0, -1):
            mult = jnp.where(sub < s, cols[s] * dinv, 0.0)
            s_sol = s_sol - mult * wide(s_sol[s:s + 1])
            m_sol = m_sol - mult * wide(m_sol[s:s + 1])
        s_rows = [wide(s_sol[t:t + 1]) for t in range(8)]
        m_rows = [wide(m_sol[t:t + 1]) for t in range(8)]
        s_new, m_new = [], []
        for v in range(1, tiles):
            s_acc, m_acc = s_tiles[v], m_tiles[v]
            for t in range(8):
                col = spread(s_tiles[v], t)
                s_acc = s_acc - col * s_rows[t]
                m_acc = m_acc - col * m_rows[t]
            s_new.append(s_acc)
            m_new.append(m_acc)
        zero = jnp.zeros((8, NB), F32)
        return tuple(s_new + [zero] + m_new + [zero])

    def tiles_of(x):
        return [x[8 * v:8 * v + 8] for v in range(x.shape[0] // 8)]

    n = NB // 8
    state = tuple(tiles_of(block) + tiles_of(eye))
    done = 0
    for tiles, steps in ((n, n // 2), (n // 2, n // 2)):
        state = lax.fori_loop(done, done + steps, functools.partial(group, tiles), state)
        done += steps
        half = len(state) // 2
        state = state[:n - done] + state[half:half + n - done]


def gram_kernel(a_hbm, s_hbm, r_ref, ok_ref, s_ref, own, peer, turned, turned_r, acc1, acc2, acc1_r, hb, cm_buf, cm_recv, cy_recv, cfin,
                xp, xp_r, xc, xt, z_buf, t_buf, rf_buf, k12, ymax, u_blk, m_blk,
                load_sem, ya_send, ya_recv, yb_send, yb_recv, yp_send, yp_recv, fs_send, fs_recv, ar_send, ar_recv, gy_send, gy_recv, gq_send, gq_recv,
                rs_send, rs_recv, cy_send, cy_rsem, ag_send, ag_recv, s_sem):
    rows, cols = a_hbm.shape
    half_rows = rows // 2
    half = cols // 2
    kk = 2 * half
    c = lax.axis_index('pcol')
    p = lax.axis_index('prow')
    other = 1 - c
    core = p % 2
    core_peer = p + 1 - 2 * core
    x_peer = (p + 2) % 4
    qr = half // 4
    qb = NB // 4
    ca = 512
    n_a = half_rows // ca
    n_l = rows // ca
    per_load = n_l // 4
    b_cuts = (0, 768, 1920, 3072)
    n_b = len(b_cuts) - 1
    starts = (0, 64, 112, NB)
    last_rows = (0, 1536, 2560, 3072)
    pieces = [(lo, hi - lo, 0, half_rows) for lo, hi in zip(starts[:-2], starts[1:-1])]
    pieces += [(starts[-2], NB - starts[-2], lo, hi - lo) for lo, hi in zip(last_rows, last_rows[1:])]
    tail = starts[-2]

    def row0(start, size):
        return pl.ds(pl.multiple_of(start, NB), size)

    def to_prow(src, dst, send, recv, q):
        return pltpu.make_async_remote_copy(src, dst, send, recv, device_id={'prow': q}, device_id_type=MESH)

    def to_pcol(src, dst, send, recv):
        return pltpu.make_async_remote_copy(src, dst, send, recv, device_id={'pcol': other}, device_id_type=MESH)

    def load(g):
        rs = row0(g * per_load * ca, per_load * ca)
        return pltpu.make_async_copy(a_hbm.at[rs, :], own.at[rs, :], load_sem.at[g])

    barrier = pltpu.get_barrier_semaphore()
    pl.semaphore_signal(barrier, inc=1, device_id={'pcol': other}, device_id_type=MESH)
    for d in range(1, 4):
        pl.semaphore_signal(barrier, inc=1, device_id={'prow': (p + d) % 4}, device_id_type=MESH)
    s_load = pltpu.make_async_copy(s_hbm, s_ref, s_sem)
    s_load.start()
    for g in range(4):
        load(g).start()
    pl.semaphore_wait(barrier, 4)

    def send_rows(start, size, lanes, send, recv):
        rs = row0(start, size)
        return to_pcol(a_hbm.at[rs, lanes], peer.at[rs, lanes], send, recv)

    def send_a(k):
        return send_rows(c * half_rows + k * ca, ca, pl.ds(0, half), ya_send, ya_recv.at[k])

    def send_b(k):
        lo, hi = b_cuts[k], b_cuts[k + 1]
        return send_rows(other * half_rows + lo, hi - lo, pl.ds(0, NB), yb_send, yb_recv.at[k])

    def send_p(i):
        col, width, lo, depth = pieces[i]
        block = (pl.ds(col, width), pl.ds(lo, depth))
        return to_pcol(turned.at[block], turned_r.at[block], yp_send, yp_recv.at[i])

    for k in range(4):
        send_a(k).start()

    eye = (lax.broadcasted_iota(jnp.int32, (NB, NB), 0) == lax.broadcasted_iota(jnp.int32, (NB, NB), 1)).astype(F32)

    def add_shift(ref, side, l, cond):
        @pl.when(jnp.logical_and(p == 0, cond))
        def _():
            panel = 2 * l + side
            rs = row0(panel * NB, NB)
            ref[rs, l * NB:(l + 1) * NB] = ref[rs, l * NB:(l + 1) * NB] + eye * s_ref[pl.ds(panel, 1), :]

    acc1[...] = jnp.zeros_like(acc1)
    acc2[...] = jnp.zeros_like(acc2)
    ymax[...] = jnp.zeros_like(ymax)
    s_load.wait()

    @pl.loop(0, n_l)
    def _(j):
        @pl.when(j % per_load == 0)
        def _():
            load(j // per_load).wait()

        for l in range(2):
            add_shift(own, c, l, j == 0)
        rs = pl.ds(pl.multiple_of(j * ca, ca), ca)
        right = own[rs, :]
        ymax[...] = jnp.maximum(ymax[...], jnp.max(jnp.abs(right[:, half:]).reshape(ca // 8, 8, half), axis=0))
        acc1[...] += dot_tn(right[:, :half], right)

    acc1[NB:NB + 8, :NB] = jnp.maximum(ymax[:, :NB], ymax[:, NB:])

    def pair_copy(src, dst, slot, q):
        return to_prow(src, dst, ar_send.at[slot], ar_recv.at[slot], q)

    g1 = pair_copy(acc1, acc1_r.at[0], 0, core_peer)
    g1.start()
    g1.wait()
    acc1[...] += acc1_r[0]
    g2 = pair_copy(acc1, acc1_r.at[1], 1, x_peer)
    g2.start()

    @pl.loop(0, half_rows // NB)
    def _(i):
        turned[:, row0(i * NB, NB)] = own[row0(other * half_rows + i * NB, NB), NB:half].T

    g2.wait()
    acc1[...] += acc1_r[1]
    for q in range(4):
        rs = slice(q * qb, (q + 1) * qb)
        hb[c, q, :qb, :] = acc1[rs, :NB]
        hb[c, q, qb:2 * qb, :] = acc1[rs, NB:half]
        hb[c, q, 2 * qb:3 * qb, :] = acc1[NB + q * qb:NB + (q + 1) * qb, NB:half]
        hb[c, q, 3 * qb:, :] = acc1[NB:NB + 8, :NB]
    gy = to_pcol(hb.at[c, p], hb.at[c, p], gy_send, gy_recv)
    gy.start()
    for k in range(4, n_a):
        send_a(k).start()
    send_b(0).start()

    def gram_block(side, b):
        return jnp.concatenate([hb[side, q, b * qb:(b + 1) * qb, :] for q in range(4)], axis=0)

    def take_a(k):
        send_a(k).wait_recv()
        for l in range(2):
            add_shift(peer, other, l, jnp.logical_and(c == 1, k == 0))
        rs = row0(other * half_rows + k * ca, ca)
        acc2[...] += dot_tn(peer[rs, :], own[rs, :])

    def spread_gram(d, src):
        return to_prow(hb.at[other, src], hb.at[other, src], gq_send.at[d - 1], gq_recv.at[d - 1], (p + d) % 4)

    @pl.loop(0, n_a)
    def _(k):
        take_a(k)

        @pl.when(k == n_a - 3)
        def _():
            gy.wait()
            for d in range(1, 4):
                spread_gram(d, p).start()

        @pl.when(k == n_a - 2)
        def _():
            for d in range(1, 4):
                spread_gram(d, p).wait_send()
                spread_gram(d, (p + 4 - d) % 4).wait_recv()
            factor_block(gram_block(0, 0), u_blk, m_blk)

    @pl.when(c == 0)
    def _():
        ct = acc2[:, :half].T
        for q in range(4):
            cm_buf[q] = ct[q * qr:(q + 1) * qr]

    @pl.when(c == 1)
    def _():
        for q in range(4):
            cm_buf[q] = acc2[q * qr:(q + 1) * qr, :half]

    def scatter(d):
        q = (p + d) % 4
        return to_prow(cm_buf.at[q], cm_recv.at[d - 1], rs_send.at[d - 1], rs_recv.at[d - 1], q)

    for d in range(1, 4):
        scatter(d).start()
    xp[...] = acc2[:NB, half:]
    xc[...] = acc2[NB:, half:]
    for d in range(1, 4):
        scatter(d).wait()
    cm_buf[p] = ((cm_buf[p] + cm_recv[0]) + cm_recv[1]) + cm_recv[2]
    cy = to_pcol(cm_buf.at[p], cy_recv, cy_send, cy_rsem)
    cy.start()
    for k in range(1, n_b):
        send_b(k).start()
    for i in range(len(pieces)):
        send_p(i).start()
    cy.wait()
    cfin[p] = cm_buf[p] + cy_recv[...]

    def spread(d, src):
        return to_prow(cfin.at[src], cfin.at[src], ag_send.at[d - 1], ag_recv.at[d - 1], (p + d) % 4)

    for d in range(1, 4):
        spread(d, p).start()
    for d in range(1, 4):
        spread(d, p).wait_send()
        spread(d, (p + 4 - d) % 4).wait_recv()

    cross = jnp.concatenate([cfin[q] for q in range(4)], axis=0)
    z_buf[...] = jnp.zeros_like(z_buf)
    diag_max = jnp.zeros((1, NB), F32)
    diag_min = jnp.full((1, NB), jnp.inf, F32)
    diags = []
    for i in range(4):
        ci, li = i % 2, i // 2
        for j in range(i, 4):
            cj, lj = j % 2, j // 2
            if ci == cj:
                block = gram_block(ci, li + lj)
            elif ci == 0:
                block = cross[li * NB:(li + 1) * NB, lj * NB:(lj + 1) * NB]
            else:
                block = cross[lj * NB:(lj + 1) * NB, li * NB:(li + 1) * NB].T
            z_buf[i * NB:(i + 1) * NB, j * NB:(j + 1) * NB] = block
            if i == j:
                d_row = jnp.sum(block * eye, axis=0, keepdims=True)
                diags.append(d_row)
                diag_max = jnp.maximum(diag_max, d_row)
                diag_min = jnp.minimum(diag_min, d_row)

    t_buf[...] = jnp.zeros_like(t_buf)
    rf_buf[...] = jnp.zeros_like(rf_buf)
    for j in range(4):
        lo, hi = j * NB, (j + 1) * NB
        if j > 0:
            factor_block(z_buf[lo:hi, lo:hi], u_blk, m_blk)
        inv_t = m_blk[...]
        rf_buf[lo:hi, lo:hi] = u_blk[...]
        t_buf[lo:hi, lo:hi] = inv_t
        new_row = dot_nn(inv_t, z_buf[lo:hi, :])
        if j > 0:
            t_buf[lo:hi, :lo] = new_row[:, :lo]
        if j < 3:
            rf_buf[lo:hi, hi:] = new_row[:, hi:]
            parts = ([new_row[:, :lo]] if j > 0 else []) + [inv_t, new_row[:, hi:]]
            mult = jnp.concatenate(parts, axis=1)
            z_buf[hi:, lo:hi] = jnp.zeros((kk - hi, NB), F32)
            z_buf[hi:, :] = z_buf[hi:, :] - dot_tn(new_row[:, hi:], mult)

    trace = jnp.zeros((1, NB), F32)
    for i in range(4):
        tc = t_buf[i * NB:, i * NB:(i + 1) * NB]
        trace = trace + jnp.sum(tc * tc, axis=0, keepdims=True) * diags[i]
    total = jnp.sum(trace, axis=1, keepdims=True)
    d_max = jnp.max(diag_max, axis=1, keepdims=True)
    d_min = jnp.min(diag_min, axis=1, keepdims=True)
    y_max = jnp.maximum(hb[0, 0, 3 * qb:, :], hb[1, 0, 3 * qb:, :])
    y_max = jnp.max(jnp.max(y_max, axis=0, keepdims=True), axis=1, keepdims=True)
    good = (total < TRACE_FACTOR * kk) & (d_min > 1e-26) & (d_max < 1e36) & (y_max * jnp.sqrt(d_max) < 1e33)
    ok_ref[0, 0] = jnp.where(good, 1, 0)[0, 0]

    for l in range(2):
        ls = pl.ds(pl.multiple_of((2 * l + c) * NB, NB), NB)
        r_ref[:, l * NB:(l + 1) * NB] = rf_buf[:, ls]

    k12[row0(c * NB, NB), :] = acc1[:NB, half:]
    k12[row0((c + 2) * NB, NB), :] = acc1[NB:, half:]
    k12[row0((3 - c) * NB, NB), :] = jnp.zeros((NB, half), F32)

    for k in range(n_b):
        send_b(k).wait_recv()
        if k == 0:
            add_shift(peer, other, 0, c == 0)
        rs = row0(c * half_rows + b_cuts[k], b_cuts[k + 1] - b_cuts[k])
        xp[...] += dot_tn(peer[rs, :NB], own[rs, half:])
    x1 = pair_copy(xp, xp_r.at[0], 2, core_peer)
    x1.start()
    x1.wait()
    xp[...] = xp[...] + xp_r[0]
    x2 = pair_copy(xp, xp_r.at[1], 3, x_peer)
    x2.start()
    x2.wait()
    k12[row0((1 - c) * NB, NB), :] = xp[...] + xp_r[1]
    r_ref[:, half:] = dot_nn(t_buf[...], k12[...])

    def take_p(i):
        col, width, lo, depth = pieces[i]
        send_p(i).wait_recv()
        step = min(depth, 1024)

        def part(start):
            xc[col:col + width, :] += dot_nn(turned_r[col:col + width, row0(start, step)], own[row0(c * half_rows + start, step), half:])

        if depth % step:
            step = depth // 3
        if depth == step:
            part(lo)
        else:
            @pl.loop(0, depth // step)
            def _(j):
                part(lo + j * step)

    def share(d, start, size, last):
        rs = pl.ds(pl.multiple_of(start, 8), size)
        return to_prow(xc.at[rs, :], xt.at[p, rs, :], fs_send.at[d - 1], fs_recv.at[last, d - 1], (p + d) % 4)

    inv_cols = t_buf[half:, pl.ds(pl.multiple_of((3 - c) * NB, NB), NB)]
    for i, (col, width, lo, depth) in enumerate(pieces):
        take_p(i)
        if lo + depth == half_rows:
            for d in range(1, 4):
                share(d, col, width, int(col == tail)).start()
    xt[p] = xc[...]
    send_rows(c * half_rows, half_rows, pl.ds(0, half), ya_send, ya_recv.at[0]).wait_send()
    send_rows(other * half_rows, half_rows, pl.ds(0, NB), yb_send, yb_recv.at[0]).wait_send()
    to_pcol(turned, turned_r, yp_send, yp_recv.at[0]).wait_send()
    for d in range(1, 4):
        share(d, 0, NB, 0).wait_send()
        share(d, 0, tail, 0).wait_recv()
    for d in range(1, 4):
        share(d, tail, NB - tail, 1).wait_recv()
    r_ref[half:, half:] += dot_nn(inv_cols, (xt[0] + xt[1]) + (xt[2] + xt[3]))


def gram_rows(a_loc, diag_shift):
    rows, cols = a_loc.shape
    half = cols // 2
    kk = cols
    qr = half // 4
    dma = pltpu.SemaphoreType.DMA
    vm = lambda *shape: pltpu.VMEM(shape, F32)
    return pl.pallas_call(
        gram_kernel,
        out_shape=(pltpu.VMEM((kk, cols), F32), pltpu.SMEM((1, 1), jnp.int32)),
        in_specs=[pl.BlockSpec(memory_space=pl.ANY), pl.BlockSpec(memory_space=pl.ANY)],
        out_specs=(pl.BlockSpec(memory_space=pltpu.VMEM), pl.BlockSpec(memory_space=pltpu.SMEM)),
        scratch_shapes=[
            vm(*diag_shift.shape), vm(rows, cols), vm(rows, half), vm(NB, rows // 2), vm(NB, rows // 2), vm(half, cols), vm(half, cols), vm(2, half, cols),
            vm(2, 4, 3 * NB // 4 + 8, NB), vm(4, qr, half), vm(3, qr, half), vm(qr, half), vm(4, qr, half),
            vm(NB, half), vm(2, NB, half), vm(NB, half), vm(4, NB, half),
            vm(kk, kk), vm(kk, kk), vm(kk, kk), vm(kk, half), vm(8, half), vm(NB, NB), vm(NB, NB),
            dma((4,)), dma, dma((rows // 1024,)), dma, dma((3,)), dma, dma((7,)), dma((3,)), dma((2, 3)), dma((4,)), dma((4,)), dma, dma, dma((3,)), dma((3,)),
            dma((3,)), dma((3,)), dma, dma, dma((3,)), dma((3,)), dma,
        ],
        compiler_params=pltpu.CompilerParams(collective_id=0, has_side_effects=True, vmem_limit_bytes=48 * 1024 * 1024),
        name='gram_rows',
    )(a_loc, diag_shift)


def solution(mesh):
    n_pcol = mesh.shape['pcol']

    def local_qr(a_loc, diag_shift):
        rows, ok = gram_rows(a_loc, diag_shift)
        return lax.cond(ok[0, 0] != 0, lambda a, s, r: r, lambda a, s, r: householder_rows(a, s, n_pcol), a_loc, diag_shift, rows)

    return jax.shard_map(local_qr, mesh=mesh, in_specs=(P(('batch', 'prow'), 'pcol'), P('batch', None)), out_specs=P('batch', 'pcol'), check_vma=False)
```
